256 devices in a mesh: seq: 128 (over y, z_lo, x, core), chan: 2 (over z_hi).
Axes of the slice: x: 4, y: 4, z: 8 (z_hi: 2, z_lo: 4; z = z_hi * 4 + z_lo), core: 2. Of those that a mesh axis runs over, the one named last changes fastest.
Arguments:
- tokens: float32 [16384, 1024], P('seq', 'chan'), may hold values from -6 to 6
- gate_weight: float32 [1024, 1024], P(None, 'chan'), may hold values from -0.1875 to 0.1875
- value_weight: float32 [1024, 1024], P(None, 'chan'), may hold values from -0.1875 to 0.1875
- output_weight: float32 [1024, 1024], P('chan'), may hold values from -0.1875 to 0.1875
- wave_numbers: int32 [32], replicated, may hold values from 1 to 2047
- position_in: float32 [64, 64], replicated, may hold values from -0.75 to 0.75
- bias_in: float32 [64], replicated, may hold values from -3 to 3
- position_mid: float32 [64, 64], replicated, may hold values from -0.75 to 0.75
- bias_mid: float32 [64], replicated, may hold values from -3 to 3
- position_out: float32 [64, 1024], P(None, 'chan'), may hold values from -1 to 1
- decay_rate: float32 [1024], P('chan'), may hold values from 0.5 to 409.6
Outputs:
- mixed_tokens: float32 [16384, 1024], P('seq', 'chan')
The draws below stay inside these ranges and needn't reach their ends.
All inputs are finite; a program needn't handle non-finite values.
Results may differ from the reference program's by a relative error of at most 0.0003.
Values sent between devices are 32-bit elements; how exact they have to be, the bound alone decides.
No kernel may reach another device: no remote copies, remote signals or barrier semaphores. Data moves between devices by JAX's collectives and lax.ppermute only.
A program may use at most 64 MiB of HBM per device.

```python
import math
import jax
import jax.numpy as jnp
from jax import lax

D = 1024
RPE_DIM = 64
PERIOD = 4096
L = 16384


def draw_tokens(key, part):
    key_a = jax.random.fold_in(jax.random.fold_in(key, 17), 0)
    return jax.random.truncated_normal(key_a, -6.0, 6.0, (L, D), jnp.float32)


def set_ends(array, stream_key, smallest, high):
    index_at = [jax.random.randint(jax.random.fold_in(stream_key, axis), (), 0, length) for axis, length in enumerate(array.shape)]
    longest = array.shape.index(max(array.shape))
    next_to = index_at[:longest] + [(index_at[longest] + 1) % array.shape[longest]] + index_at[longest + 1:]
    return array.at[tuple(index_at)].set(smallest).at[tuple(next_to)].set(high)


def block_scale(key, dims, shards, low, top_value):
    loudness = 1.0
    for axis_at, blocks in shards:
        draws = jax.random.uniform(jax.random.fold_in(jax.random.fold_in(key, 6), axis_at), (blocks,), jnp.float32, low / len(shards), top_value / len(shards))
        loudness = loudness * jnp.repeat(jnp.exp(draws), dims[axis_at] // blocks).reshape((-1,) + (1,) * (len(dims) - 1 - axis_at))
    return loudness


def centred(rng, extent, deviation, most, cuts=(), held_as=jnp.bfloat16):
    factor_of = block_scale(rng, extent, cuts, -0.22, 0.18) if cuts else 1.0
    drawn = jax.random.normal(rng, extent, jnp.float32) * deviation * factor_of
    return jnp.minimum(jnp.maximum(drawn, -most), most).astype(held_as)


def setup_inputs(seed: int = 0) -> dict:
    splits = jax.random.split(jax.random.key(seed), 12)
    return {
        "tokens": draw_tokens(jax.random.fold_in(splits[11], 71), 0),
        "gate_weight": centred(splits[1], (D, D), D ** -0.5, 0.1875, ((1, 2),), jnp.float32),
        "value_weight": centred(splits[2], (D, D), D ** -0.5, 0.1875, ((1, 2),), jnp.float32),
        "output_weight": centred(splits[3], (D, D), D ** -0.5, 0.1875, ((0, 2),), jnp.float32),
        "wave_numbers": set_ends(jax.random.randint(splits[4], (RPE_DIM // 2,), 1, PERIOD // 2), jax.random.fold_in(splits[4], 1), 1, (PERIOD // 2) - 1).astype(jnp.int32),
        "position_in": centred(splits[5], (RPE_DIM, RPE_DIM), RPE_DIM ** -0.5, 0.75, (), jnp.float32),
        "bias_in": centred(splits[6], (RPE_DIM,), 0.5, 3.0, (), jnp.float32),
        "position_mid": centred(splits[7], (RPE_DIM, RPE_DIM), RPE_DIM ** -0.5, 0.75, (), jnp.float32),
        "bias_mid": centred(splits[8], (RPE_DIM,), 0.5, 3.0, (), jnp.float32),
        "position_out": centred(splits[9], (RPE_DIM, D), (RPE_DIM // 2) ** -0.5, 1.0, ((1, 2),), jnp.float32),
        "decay_rate": jnp.clip(jnp.exp(math.log(409.6) - 6.7083283 * jax.random.uniform(splits[10], (D,), jnp.float32) ** block_scale(splits[10], (D,), ((0, 2),), -0.2, 0.2)), 0.5, 409.6),
    }


HIGHEST = lax.Precision.HIGHEST

def position_net(positions, wave_numbers, position_in, bias_in, position_mid, bias_mid, position_out, decay_rate, seq_length):
    phases = (positions % PERIOD)[:, None] * wave_numbers[None, :] % PERIOD
    angles = phases.astype(jnp.float32) * (2.0 * math.pi / PERIOD)
    features = jnp.concatenate([jnp.cos(angles), jnp.sin(angles)], axis=1)
    hidden = jax.nn.relu(jnp.dot(features, position_in, precision=HIGHEST) + bias_in)
    hidden = jax.nn.relu(jnp.dot(hidden, position_mid, precision=HIGHEST) + bias_mid)
    shapes = jnp.dot(hidden, position_out, precision=HIGHEST)
    spots = positions.astype(jnp.float32) / seq_length
    envelope = jnp.exp(-decay_rate[None, :] * spots[:, None]) * jnp.sqrt(2.0 * decay_rate / seq_length)[None, :]
    return shapes * envelope

def reference(tokens, gate_weight, value_weight, output_weight, wave_numbers, position_in, bias_in, position_mid, bias_mid, position_out, decay_rate):
    seq_length = tokens.shape[0]
    gated = jax.nn.silu(jnp.dot(tokens, gate_weight, precision=HIGHEST))
    values = jax.nn.silu(jnp.dot(tokens, value_weight, precision=HIGHEST))
    positions = jnp.arange(seq_length, dtype=jnp.int32)
    kernel = position_net(positions, wave_numbers, position_in, bias_in, position_mid, bias_mid, position_out, decay_rate, seq_length)
    padded_length = 2 * seq_length
    spectrum = jnp.fft.rfft(values, n=padded_length, axis=0) * jnp.fft.rfft(kernel, n=padded_length, axis=0)
    conv = jnp.fft.irfft(spectrum, n=padded_length, axis=0)[:seq_length]
    return jnp.dot(gated * conv, output_weight, precision=HIGHEST)
```

```python
import math

import jax
import jax.numpy as jnp
import numpy as np
from jax import lax
from jax.experimental import pallas as pl
from jax.experimental.pallas import tpu as pltpu
from jax.sharding import PartitionSpec as P

PERIOD = 4096
F32 = jnp.float32
BF16 = jnp.bfloat16


def split(value):
    high = value.astype(BF16)
    low = (value - high.astype(F32)).astype(BF16)
    return high, low


def split_table(table):
    high = table.astype(np.float32).astype(jnp.bfloat16)
    low = (table - high.astype(np.float64)).astype(np.float32).astype(jnp.bfloat16)
    return high, low


def matmul(left, right):
    return jnp.dot(left, right, preferred_element_type=F32)


def dot3(left, right):
    left_high, left_low = left
    right_high, right_low = right
    return (
        matmul(left_high, right_low)
        + matmul(left_low, right_high)
        + matmul(left_high, right_high)
    )


def silu(value):
    return value / (1.0 + jnp.exp(-value))


def fourier_tables(outer, inner):
    n1 = np.arange(outer)
    n2 = np.arange(inner)
    angle = 2.0 * np.pi * ((n1[:, None] * n1[None, :]) % outer) / outer
    cos1, sin1 = np.cos(angle), np.sin(angle)
    first = np.block([[cos1, sin1], [-sin1, cos1]])
    half = outer // 2
    last = np.block([[cos1[half:], -sin1[half:]], [sin1[half:], cos1[half:]]])
    angle = 2.0 * np.pi * ((n2[:, None] * n2[None, :]) % inner) / inner
    cos2, sin2 = np.cos(angle), np.sin(angle)
    second = np.block([[cos2, -sin2], [sin2, cos2]])
    angle = 2.0 * np.pi * (n1[:, None] * n2[None, :]) / (outer * inner)
    turn = np.stack([np.cos(angle), -np.sin(angle)]).astype(np.float32)
    return first, second, last, turn


def call(kernel, out_shapes, scratch=(), flops=0, *, name):
    vmem = pl.BlockSpec(memory_space=pltpu.VMEM)
    many = isinstance(out_shapes, (list, tuple))
    return pl.pallas_call(
        kernel,
        out_shape=out_shapes,
        out_specs=[vmem] * len(out_shapes) if many else vmem,
        scratch_shapes=list(scratch),
        name=name,
        compiler_params=pltpu.CompilerParams(vmem_limit_bytes=48 << 20),
        cost_estimate=pl.CostEstimate(flops=flops, transcendentals=0, bytes_accessed=0),
    )


def spectrum_kernel(
    cos_a, sin_a, cos_b, sin_b, in_w, in_b, mid_w, mid_b, out_w, decay, first, first_low, second, second_low, turn,
    spec_real, spec_imag, features, shapes, *, seq_length
):
    near, lanes = cos_a.shape[1], cos_b.shape[1]
    waves = cos_a.shape[0]
    chans = spec_real.shape[0] // turn.shape[1]
    for at in range(near):
        here = slice(at * lanes, (at + 1) * lanes)
        cos_at, sin_at = cos_a[:, at : at + 1], sin_a[:, at : at + 1]
        features[:waves, here] = cos_at * cos_b[...] - sin_at * sin_b[...]
        features[waves:, here] = sin_at * cos_b[...] + cos_at * sin_b[...]
    hidden = jnp.maximum(dot3(split(in_w[...]), split(features[...])) + in_b[...], 0.0)
    hidden = jnp.maximum(dot3(split(mid_w[...]), split(hidden)) + mid_b[...], 0.0)
    lines = dot3(split(out_w[...]), split(hidden))
    pad = lines.shape[0]
    for at in range(near):
        shapes[at * pad : (at + 1) * pad, :] = lines[:, at * lanes : (at + 1) * lanes]
    spots = (
        lax.broadcasted_iota(jnp.int32, (near, lanes), 0) * lanes
        + lax.broadcasted_iota(jnp.int32, (near, lanes), 1)
    ).astype(F32) / seq_length
    kernels = []
    for chan in range(chans):
        rate = decay[chan : chan + 1, :]
        envelope = jnp.exp(-rate * spots) * jnp.sqrt(2.0 * rate / seq_length)
        kernels.append(shapes[pl.ds(chan, near, stride=pad), :] * envelope)
    outer = turn.shape[1]
    grid = jnp.concatenate(kernels, axis=1)
    forms = dot3((first[:, :near], first_low[:, :near]), split(grid))
    rows = []
    for chan in range(chans):
        here = slice(chan * lanes, (chan + 1) * lanes)
        real, imag = forms[:outer, here], forms[outer:, here]
        rows.append(
            jnp.concatenate(
                [real * turn[0] - imag * turn[1], real * turn[1] + imag * turn[0]], axis=1
            )
        )
    spec = dot3(split(jnp.concatenate(rows, axis=0)), (second[...], second_low[...]))
    scale = 1.0 / (outer * lanes)
    spec_real[...] = spec[:, :lanes] * scale
    spec_imag[...] = spec[:, lanes:] * scale


def convolve_kernel(
    values, spec_real, spec_imag, decay, first, first_low, second, second_low, back, back_low, last, last_low, turn,
    out, *, ratio
):
    outer, lanes = turn.shape[1], turn.shape[2]
    near = outer // 2
    chans = spec_real.shape[0] // outer
    peers = values.shape[0] // chans
    blocks = peers // near
    pairs = blocks // 2
    columns = []
    for chan in range(chans):
        lines = values[pl.ds(chan, peers, stride=chans), :]
        keep = jnp.exp(-decay[chan : chan + 1, :] * ratio)
        carried = [jnp.zeros((near, lanes), F32), lines[:near]]
        for block in range(1, blocks):
            carried.append(lines[block * near : (block + 1) * near] + keep * carried[-1])
        for pair in range(pairs):
            low = 2 * pair
            columns.append(
                jnp.concatenate(
                    [carried[low], carried[low + 1], carried[low + 1], carried[low + 2]], axis=0
                )
            )
    forms = dot3((first[...], first_low[...]), split(jnp.concatenate(columns, axis=1)))
    turn_real, turn_imag = turn[0], turn[1]
    rows = []
    for at in range(chans * pairs):
        here = slice(at * lanes, (at + 1) * lanes)
        real, imag = forms[:outer, here], forms[outer:, here]
        rows.append(
            jnp.concatenate(
                [real * turn_real - imag * turn_imag, real * turn_imag + imag * turn_real], axis=1
            )
        )
    spec = dot3(split(jnp.concatenate(rows, axis=0)), (second[...], second_low[...]))
    rows = []
    for at in range(chans * pairs):
        chan = at // pairs
        real = spec[at * outer : (at + 1) * outer, :lanes]
        imag = spec[at * outer : (at + 1) * outer, lanes:]
        k_real = spec_real[chan * outer : (chan + 1) * outer, :]
        k_imag = spec_imag[chan * outer : (chan + 1) * outer, :]
        rows.append(
            jnp.concatenate(
                [real * k_real - imag * k_imag, real * k_imag + imag * k_real], axis=1
            )
        )
    forms = dot3(split(jnp.concatenate(rows, axis=0)), (back[...], back_low[...]))
    columns = []
    for at in range(chans * pairs):
        real = forms[at * outer : (at + 1) * outer, :lanes]
        imag = forms[at * outer : (at + 1) * outer, lanes:]
        columns.append(
            jnp.concatenate(
                [real * turn_real + imag * turn_imag, imag * turn_real - real * turn_imag], axis=0
            )
        )
    lines = dot3((last[...], last_low[...]), split(jnp.concatenate(columns, axis=1)))
    for chan in range(chans):
        both = [
            lines[:, (chan * pairs + pair) * lanes : (chan * pairs + pair + 1) * lanes]
            for pair in range(pairs)
        ]
        out[pl.ds(chan, peers, stride=chans), :] = jnp.concatenate(both, axis=0)


def prepare_kernel(
    tokens, gate_w, value_w, out_w,
    value_sum, gate_sum, value_high, value_low, gate_high, gate_low, send_high, send_low, keep_high, keep_low
):
    width = tokens.shape[1]
    me = lax.axis_index("chan")
    mine = pl.ds(pl.multiple_of(me * width, width), width)
    other = pl.ds(pl.multiple_of((1 - me) * width, width), width)
    own = split(tokens[...])
    value_sum[...] = dot3(own, split(value_w[mine, :]))
    gate_sum[...] = dot3(own, split(gate_w[mine, :]))
    value_high[...], value_low[...] = split(value_w[other, :])
    gate_high[...], gate_low[...] = split(gate_w[other, :])
    send_high[...], send_low[...] = split(out_w[:, other])
    keep_high[...], keep_low[...] = split(out_w[:, mine])


def value_kernel(tokens, partial, w_high, w_low, out):
    out[...] = silu(partial[...] + dot3(split(tokens[...]), (w_high[...], w_low[...]))).T


def gate_kernel(tokens, partial, w_high, w_low, out):
    out[...] = silu(partial[...] + dot3(split(tokens[...]), (w_high[...], w_low[...])))


def send_kernel(conv, gated, w_high, w_low, out, term_high, term_low):
    terms = split(gated[...] * conv[...].T)
    term_high[...], term_low[...] = terms
    out[...] = dot3(terms, (w_high[...], w_low[...]))


def keep_kernel(term_high, term_low, w_high, w_low, out):
    out[...] = dot3((term_high[...], term_low[...]), (w_high[...], w_low[...]))


def angle_tables(steps, wave_numbers):
    phases = wave_numbers[:, None] * steps[None, :] % PERIOD
    angles = phases.astype(F32) * (2.0 * math.pi / PERIOD)
    return jnp.cos(angles), jnp.sin(angles)


def on_device(
    tokens,
    gate_weight,
    value_weight,
    output_weight,
    wave_numbers,
    position_in,
    bias_in,
    position_mid,
    bias_mid,
    position_out,
    decay_rate,
):
    peer_count = lax.axis_size("seq")
    row_count, local_width = tokens.shape
    seq_length = row_count * peer_count
    chans = local_width // peer_count
    near = PERIOD // row_count
    outer = 2 * near
    swap = [(0, 1), (1, 0)]
    other_tokens = lax.ppermute(tokens, "chan", swap)

    first, second, last, turn = fourier_tables(outer, row_count)
    first_h, first_l = split_table(first)
    second_h, second_l = split_table(second)
    back_h, back_l = split_table(second.T)
    last_h, last_l = split_table(last)

    first_chan = lax.axis_index("seq") * chans
    own_out = lax.dynamic_slice_in_dim(position_out, first_chan, chans, 1)
    own_out = jnp.pad(own_out.T, ((0, 8 - chans), (0, 0)))
    own_decay = lax.dynamic_slice_in_dim(decay_rate, first_chan, chans, 0)
    own_decay = jnp.broadcast_to(own_decay[:, None], (chans, row_count))
    cos_a, sin_a = angle_tables(jnp.arange(near, dtype=jnp.int32) * row_count, wave_numbers)
    cos_b, sin_b = angle_tables(jnp.arange(row_count, dtype=jnp.int32), wave_numbers)

    def shaped(*dims, dtype=F32):
        return jax.ShapeDtypeStruct(dims, dtype)

    width = position_in.shape[0]
    spec_real, spec_imag = call(
        lambda *refs: spectrum_kernel(*refs, seq_length=seq_length),
        [shaped(chans * outer, row_count)] * 2,
        [pltpu.VMEM((width, PERIOD), F32), pltpu.VMEM((8 * near, row_count), F32)],
        10**9,
        name="spectrum",
    )(
        cos_a, sin_a, cos_b, sin_b, position_in.T, bias_in[:, None], position_mid.T, bias_mid[:, None], own_out,
        own_decay, first_h, first_l, second_h, second_l, turn,
    )
    block = shaped(local_width, local_width, dtype=BF16)
    rows = shaped(row_count, local_width)
    (
        value_sum, gate_sum, value_high, value_low, gate_high, gate_low, send_high, send_low, keep_high, keep_low,
    ) = call(prepare_kernel, [rows, rows] + [block] * 8, flops=10**9, name="prepare")(
        tokens, gate_weight, value_weight, output_weight
    )
    flat = shaped(local_width, row_count)
    values = call(value_kernel, flat, flops=10**8, name="value")(
        other_tokens, value_sum, value_high, value_low
    )
    value_lines = lax.all_to_all(values, "seq", split_axis=0, concat_axis=0, tiled=True)
    gated = call(gate_kernel, rows, flops=10**8, name="gate")(
        other_tokens, gate_sum, gate_high, gate_low
    )
    conv_lines = call(
        lambda *refs: convolve_kernel(*refs, ratio=PERIOD / seq_length), flat, flops=10**9, name="convolve"
    )(
        value_lines, spec_real, spec_imag, own_decay, first_h, first_l, second_h, second_l, back_h, back_l,
        last_h, last_l, turn,
    )
    conv = lax.all_to_all(conv_lines, "seq", split_axis=0, concat_axis=0, tiled=True)
    term = shaped(row_count, local_width, dtype=BF16)
    sent, term_high, term_low = call(send_kernel, [rows, term, term], flops=10**8, name="send")(
        conv, gated, send_high, send_low
    )
    received = lax.ppermute(sent, "chan", swap)
    kept = call(keep_kernel, rows, flops=10**8, name="keep")(term_high, term_low, keep_high, keep_low)
    return kept + received


def solution(mesh):
    placed = (
        P("seq", "chan"),
        P(None, "chan"),
        P(None, "chan"),
        P("chan", None),
        P(),
        P(),
        P(),
        P(),
        P(),
        P(None, "chan"),
        P("chan"),
    )
    return jax.shard_map(
        on_device, mesh=mesh, in_specs=placed, out_specs=P("seq", "chan"), check_vma=False
    )
```

```python
import math

import jax
import jax.numpy as jnp
import numpy as np
from jax import lax
from jax.experimental import pallas as pl
from jax.experimental.pallas import tpu as pltpu
from jax.sharding import PartitionSpec as P

PERIOD = 4096
F32 = jnp.float32
BF16 = jnp.bfloat16


def split(value):
    high = value.astype(BF16)
    low = (value - high.astype(F32)).astype(BF16)
    return high, low


def split_table(table):
    high = table.astype(np.float32).astype(jnp.bfloat16)
    low = (table - high.astype(np.float64)).astype(np.float32).astype(jnp.bfloat16)
    return high, low


def matmul(left, right):
    return jnp.dot(left, right, preferred_element_type=F32)


def dot3(left, right):
    left_high, left_low = left
    right_high, right_low = right
    return (
        matmul(left_high, right_low)
        + matmul(left_low, right_high)
        + matmul(left_high, right_high)
    )


def silu(value):
    return value / (1.0 + jnp.exp(-value))


def fourier_tables(outer, inner):
    n1 = np.arange(outer)
    n2 = np.arange(inner)
    angle = 2.0 * np.pi * ((n1[:, None] * n1[None, :]) % outer) / outer
    cos1, sin1 = np.cos(angle), np.sin(angle)
    first = np.block([[cos1, sin1], [-sin1, cos1]])
    half = outer // 2
    last = np.block([[cos1[half:], -sin1[half:]], [sin1[half:], cos1[half:]]])
    angle = 2.0 * np.pi * ((n2[:, None] * n2[None, :]) % inner) / inner
    cos2, sin2 = np.cos(angle), np.sin(angle)
    second = np.block([[cos2, -sin2], [sin2, cos2]])
    angle = 2.0 * np.pi * (n1[:, None] * n2[None, :]) / (outer * inner)
    turn = np.stack([np.cos(angle), -np.sin(angle)]).astype(np.float32)
    return first, second, last, turn


def call(kernel, out_shapes, scratch=(), flops=0, scalars=(), *, name):
    vmem = pl.BlockSpec(memory_space=pltpu.VMEM)
    smem = pl.BlockSpec(memory_space=pltpu.SMEM)
    many = isinstance(out_shapes, (list, tuple))

    def run(*args):
        return pl.pallas_call(
            kernel,
            out_shape=out_shapes,
            in_specs=[smem if at in scalars else vmem for at in range(len(args))],
            out_specs=[vmem] * len(out_shapes) if many else vmem,
            scratch_shapes=list(scratch),
            name=name,
            compiler_params=pltpu.CompilerParams(vmem_limit_bytes=48 << 20),
            cost_estimate=pl.CostEstimate(flops=flops, transcendentals=0, bytes_accessed=0),
        )(*args)

    return run


def spectrum_kernel(
    cos_a, sin_a, cos_b, sin_b, in_w, in_b, mid_w, mid_b, out_w, decay, first, first_low, second, second_low, turn,
    spec_real, spec_imag, features, shapes, layer, *, seq_length
):
    near, lanes = cos_a.shape[1], cos_b.shape[1]
    waves, width = cos_a.shape[0], in_w.shape[0]
    outer = turn.shape[1]
    chans = spec_real.shape[0] // outer
    me = lax.axis_index("seq")
    pad = 8
    for at in range(near):
        here = slice(at * lanes, (at + 1) * lanes)
        cos_at, sin_at = cos_a[:, at : at + 1], sin_a[:, at : at + 1]
        features[:waves, here] = cos_at * cos_b[...] - sin_at * sin_b[...]
        features[waves:, here] = sin_at * cos_b[...] + cos_at * sin_b[...]
    one = (lax.broadcasted_iota(jnp.int32, (pad, PERIOD), 0) == 0).astype(F32)

    def dense(weight, bias, value):
        layer[...] = jnp.zeros_like(layer)
        layer[:width, :width] = weight[...]
        layer[width : width + 1, :width] = bias[...]
        turned = layer[...].T[:width, : width + pad]
        return jnp.maximum(dot3(split(turned), split(jnp.concatenate([value, one], axis=0))), 0.0)

    hidden = dense(in_w, in_b, features[...])
    hidden = dense(mid_w, mid_b, hidden)
    per_tile = lanes // chans
    tile = out_w[:, pl.ds(pl.multiple_of(me // per_tile * lanes, lanes), lanes)]
    own = pltpu.roll(tile, lanes - me % per_tile * chans, 1).T[:pad, :]
    lines = dot3(split(own), split(hidden))
    for at in range(near):
        shapes[at * pad : (at + 1) * pad, :] = lines[:, at * lanes : (at + 1) * lanes]
    spots = (
        lax.broadcasted_iota(jnp.int32, (near, lanes), 0) * lanes
        + lax.broadcasted_iota(jnp.int32, (near, lanes), 1)
    ).astype(F32) / seq_length
    kernels = []
    for chan in range(chans):
        rate = jnp.full((near, lanes), decay[me * chans + chan], F32)
        envelope = jnp.exp(-rate * spots) * jnp.sqrt(2.0 * rate / seq_length)
        kernels.append(shapes[pl.ds(chan, near, stride=pad), :] * envelope)
    grid = jnp.concatenate(kernels, axis=1)
    forms = dot3((first[:, :near], first_low[:, :near]), split(grid))
    rows = []
    for chan in range(chans):
        here = slice(chan * lanes, (chan + 1) * lanes)
        real, imag = forms[:outer, here], forms[outer:, here]
        rows.append(
            jnp.concatenate(
                [real * turn[0] - imag * turn[1], real * turn[1] + imag * turn[0]], axis=1
            )
        )
    spec = dot3(split(jnp.concatenate(rows, axis=0)), (second[...], second_low[...]))
    scale = 1.0 / (outer * lanes)
    spec_real[...] = spec[:, :lanes] * scale
    spec_imag[...] = spec[:, lanes:] * scale


def convolve_kernel(
    values, spec_real, spec_imag, decay, first, first_low, second, second_low, back, back_low, last, last_low, turn,
    out, *, ratio
):
    outer, lanes = turn.shape[1], turn.shape[2]
    near = outer // 2
    chans = spec_real.shape[0] // outer
    peers = values.shape[0] // chans
    blocks = peers // near
    pairs = blocks // 2
    columns = []
    for chan in range(chans):
        lines = values[pl.ds(chan, peers, stride=chans), :]
        rate = jnp.full((1, lanes), decay[lax.axis_index("seq") * chans + chan], F32)
        keep = jnp.exp(-rate * ratio)
        carried = [jnp.zeros((near, lanes), F32), lines[:near]]
        for block in range(1, blocks):
            carried.append(lines[block * near : (block + 1) * near] + keep * carried[-1])
        for pair in range(pairs):
            low = 2 * pair
            columns.append(
                jnp.concatenate(
                    [carried[low], carried[low + 1], carried[low + 1], carried[low + 2]], axis=0
                )
            )
    forms = dot3((first[...], first_low[...]), split(jnp.concatenate(columns, axis=1)))
    turn_real, turn_imag = turn[0], turn[1]
    rows = []
    for at in range(chans * pairs):
        here = slice(at * lanes, (at + 1) * lanes)
        real, imag = forms[:outer, here], forms[outer:, here]
        rows.append(
            jnp.concatenate(
                [real * turn_real - imag * turn_imag, real * turn_imag + imag * turn_real], axis=1
            )
        )
    spec = dot3(split(jnp.concatenate(rows, axis=0)), (second[...], second_low[...]))
    rows = []
    for at in range(chans * pairs):
        chan = at // pairs
        real = spec[at * outer : (at + 1) * outer, :lanes]
        imag = spec[at * outer : (at + 1) * outer, lanes:]
        k_real = spec_real[chan * outer : (chan + 1) * outer, :]
        k_imag = spec_imag[chan * outer : (chan + 1) * outer, :]
        rows.append(
            jnp.concatenate(
                [real * k_real - imag * k_imag, real * k_imag + imag * k_real], axis=1
            )
        )
    forms = dot3(split(jnp.concatenate(rows, axis=0)), (back[...], back_low[...]))
    columns = []
    for at in range(chans * pairs):
        real = forms[at * outer : (at + 1) * outer, :lanes]
        imag = forms[at * outer : (at + 1) * outer, lanes:]
        columns.append(
            jnp.concatenate(
                [real * turn_real + imag * turn_imag, imag * turn_real - real * turn_imag], axis=0
            )
        )
    lines = dot3((last[...], last_low[...]), split(jnp.concatenate(columns, axis=1)))
    for chan in range(chans):
        both = [
            lines[:, (chan * pairs + pair) * lanes : (chan * pairs + pair + 1) * lanes]
            for pair in range(pairs)
        ]
        out[pl.ds(chan, peers, stride=chans), :] = jnp.concatenate(both, axis=0)


def prepare_kernel(
    tokens, gate_w, value_w, out_w,
    value_sum, gate_sum, value_high, value_low, gate_high, gate_low, send_high, send_low, keep_high, keep_low
):
    width = tokens.shape[1]
    me = lax.axis_index("chan")
    mine = pl.ds(pl.multiple_of(me * width, width), width)
    other = pl.ds(pl.multiple_of((1 - me) * width, width), width)
    own = split(tokens[...])
    value_sum[...] = dot3(own, split(value_w[mine, :]))
    gate_sum[...] = dot3(own, split(gate_w[mine, :]))
    value_high[...], value_low[...] = split(value_w[other, :])
    gate_high[...], gate_low[...] = split(gate_w[other, :])
    send_high[...], send_low[...] = split(out_w[:, other])
    keep_high[...], keep_low[...] = split(out_w[:, mine])


def fold_kernel(tokens, value_in, gate_in, value_high, value_low, gate_high, gate_low, value_sum, gate_sum):
    depth = tokens.shape[1]
    terms = split(tokens[...])
    value_sum[...] = value_in[...] + dot3(terms, (value_high[:depth, :], value_low[:depth, :]))
    gate_sum[...] = gate_in[...] + dot3(terms, (gate_high[:depth, :], gate_low[:depth, :]))


def project_kernel(tokens, value_in, gate_in, value_high, value_low, gate_high, gate_low, values, gated):
    depth = tokens.shape[1]
    terms = split(tokens[...])
    values[...] = silu(value_in[...] + dot3(terms, (value_high[depth:, :], value_low[depth:, :]))).T
    gated[...] = silu(gate_in[...] + dot3(terms, (gate_high[depth:, :], gate_low[depth:, :])))


def send_kernel(conv, gated, w_high, w_low, out, term_high, term_low):
    depth = out.shape[1]
    terms = split(gated[...] * conv[...].T)
    term_high[...], term_low[...] = terms
    out[...] = dot3(terms, (w_high[:, :depth], w_low[:, :depth]))


def rest_kernel(term_high, term_low, w_high, w_low, out):
    depth = out.shape[1]
    out[...] = dot3((term_high[...], term_low[...]), (w_high[:, -depth:], w_low[:, -depth:]))


def angle_tables(steps, wave_numbers):
    phases = wave_numbers[:, None] * steps[None, :] % PERIOD
    angles = phases.astype(F32) * (2.0 * math.pi / PERIOD)
    return jnp.cos(angles), jnp.sin(angles)


def on_device(
    tokens,
    gate_weight,
    value_weight,
    output_weight,
    wave_numbers,
    position_in,
    bias_in,
    position_mid,
    bias_mid,
    position_out,
    decay_rate,
):
    peer_count = lax.axis_size("seq")
    row_count, local_width = tokens.shape
    seq_length = row_count * peer_count
    chans = local_width // peer_count
    near = PERIOD // row_count
    outer = 2 * near
    swap = [(0, 1), (1, 0)]
    half = local_width // 2
    other_first = lax.ppermute(tokens[:, :half], "chan", swap)
    other_second = lax.ppermute(tokens[:, half:], "chan", swap)

    first, second, last, turn = fourier_tables(outer, row_count)
    first_h, first_l = split_table(first)
    second_h, second_l = split_table(second)
    back_h, back_l = split_table(second.T)
    last_h, last_l = split_table(last)

    cos_a, sin_a = angle_tables(jnp.arange(near, dtype=jnp.int32) * row_count, wave_numbers)
    cos_b, sin_b = angle_tables(jnp.arange(row_count, dtype=jnp.int32), wave_numbers)

    def shaped(*dims, dtype=F32):
        return jax.ShapeDtypeStruct(dims, dtype)

    width = position_in.shape[0]
    spec_real, spec_imag = call(
        lambda *refs: spectrum_kernel(*refs, seq_length=seq_length),
        [shaped(chans * outer, row_count)] * 2,
        [
            pltpu.VMEM((width, PERIOD), F32),
            pltpu.VMEM((8 * near, row_count), F32),
            pltpu.VMEM((row_count, row_count), F32),
        ],
        10**9,
        scalars={9},
        name="spectrum",
    )(
        cos_a, sin_a, cos_b, sin_b, position_in, bias_in[None, :], position_mid, bias_mid[None, :], position_out,
        decay_rate, first_h, first_l, second_h, second_l, turn,
    )
    block = shaped(local_width, local_width, dtype=BF16)
    rows = shaped(row_count, local_width)
    half_rows = shaped(row_count, half)
    prepared = call(prepare_kernel, [rows, rows] + [block] * 8, flops=10**9, name="prepare")(
        tokens, gate_weight, value_weight, output_weight
    )
    other_first, spec_real, spec_imag, prepared = lax.optimization_barrier(
        (other_first, spec_real, spec_imag, prepared)
    )
    (
        value_sum, gate_sum, value_high, value_low, gate_high, gate_low, send_high, send_low, keep_high, keep_low,
    ) = prepared
    weights = (value_high, value_low, gate_high, gate_low)
    value_sum, gate_sum = call(fold_kernel, [rows, rows], flops=10**8, name="fold")(
        other_first, value_sum, gate_sum, *weights
    )
    flat = shaped(local_width, row_count)
    values, gated = call(project_kernel, [flat, rows], flops=10**8, name="project")(
        other_second, value_sum, gate_sum, *weights
    )
    value_lines = lax.all_to_all(values, "seq", split_axis=0, concat_axis=0, tiled=True)
    conv_lines = call(
        lambda *refs: convolve_kernel(*refs, ratio=PERIOD / seq_length), flat, flops=10**9, scalars={3},
        name="convolve",
    )(
        value_lines, spec_real, spec_imag, decay_rate, first_h, first_l, second_h, second_l, back_h, back_l,
        last_h, last_l, turn,
    )
    conv = lax.all_to_all(conv_lines, "seq", split_axis=0, concat_axis=0, tiled=True)
    term = shaped(row_count, local_width, dtype=BF16)
    sent, term_high, term_low = call(send_kernel, [half_rows, term, term], flops=10**8, name="send")(
        conv, gated, send_high, send_low
    )
    received_first = lax.ppermute(sent, "chan", swap)
    sent = call(rest_kernel, half_rows, flops=10**8, name="rest")(term_high, term_low, send_high, send_low)
    received_second = lax.ppermute(sent, "chan", swap)
    kept = call(rest_kernel, rows, flops=10**8, name="keep")(term_high, term_low, keep_high, keep_low)
    return kept + jnp.concatenate([received_first, received_second], axis=1)


def solution(mesh):
    placed = (
        P("seq", "chan"),
        P(None, "chan"),
        P(None, "chan"),
        P("chan", None),
        P(),
        P(),
        P(),
        P(),
        P(),
        P(None, "chan"),
        P("chan"),
    )
    return jax.shard_map(
        on_device, mesh=mesh, in_specs=placed, out_specs=P("seq", "chan"), check_vma=False
    )
```

```python
import math

import jax
import jax.numpy as jnp
import numpy as np
from jax import lax
from jax.experimental import pallas as pl
from jax.experimental.pallas import tpu as pltpu
from jax.sharding import PartitionSpec as P

PERIOD = 4096
F32 = jnp.float32
BF16 = jnp.bfloat16


def split(value):
    high = value.astype(BF16)
    low = (value - high.astype(F32)).astype(BF16)
    return high, low


def split_table(table):
    high = table.astype(np.float32).astype(jnp.bfloat16)
    low = (table - high.astype(np.float64)).astype(np.float32).astype(jnp.bfloat16)
    return high, low


def matmul(left, right):
    return jnp.dot(left, right, preferred_element_type=F32)


def dot3(left, right):
    left_high, left_low = left
    right_high, right_low = right
    return (
        matmul(left_high, right_low)
        + matmul(left_low, right_high)
        + matmul(left_high, right_high)
    )


def silu(value):
    return value / (1.0 + jnp.exp(-value))


def fourier_tables(outer, inner):
    n1 = np.arange(outer)
    n2 = np.arange(inner)
    angle = 2.0 * np.pi * ((n1[:, None] * n1[None, :]) % outer) / outer
    cos1, sin1 = np.cos(angle), np.sin(angle)
    first = np.block([[cos1, sin1], [-sin1, cos1]])
    half = outer // 2
    last = np.block([[cos1[half:], -sin1[half:]], [sin1[half:], cos1[half:]]])
    angle = 2.0 * np.pi * ((n2[:, None] * n2[None, :]) % inner) / inner
    cos2, sin2 = np.cos(angle), np.sin(angle)
    second = np.block([[cos2, -sin2], [sin2, cos2]])
    angle = 2.0 * np.pi * (n1[:, None] * n2[None, :]) / (outer * inner)
    turn = np.stack([np.cos(angle), -np.sin(angle)]).astype(np.float32)
    return first, second, last, turn


def call(kernel, out_shapes, scratch=(), flops=0, scalars=(), *, name):
    vmem = pl.BlockSpec(memory_space=pltpu.VMEM)
    smem = pl.BlockSpec(memory_space=pltpu.SMEM)
    many = isinstance(out_shapes, (list, tuple))

    def run(*args):
        return pl.pallas_call(
            kernel,
            out_shape=out_shapes,
            in_specs=[smem if at in scalars else vmem for at in range(len(args))],
            out_specs=[vmem] * len(out_shapes) if many else vmem,
            scratch_shapes=list(scratch),
            name=name,
            compiler_params=pltpu.CompilerParams(vmem_limit_bytes=48 << 20),
            cost_estimate=pl.CostEstimate(flops=flops, transcendentals=0, bytes_accessed=0),
        )(*args)

    return run


def spectrum_kernel(
    cos_a, sin_a, cos_b, sin_b, in_w, in_b, mid_w, mid_b, out_w, decay, first, first_low, second, second_low, turn,
    spec_real, spec_imag, features, shapes, layer, *, seq_length
):
    near, lanes = cos_a.shape[1], cos_b.shape[1]
    waves, width = cos_a.shape[0], in_w.shape[0]
    outer = turn.shape[1]
    chans = spec_real.shape[0] // outer
    me = lax.axis_index("seq")
    pad = 8
    for at in range(near):
        here = slice(at * lanes, (at + 1) * lanes)
        cos_at, sin_at = cos_a[:, at : at + 1], sin_a[:, at : at + 1]
        features[:waves, here] = cos_at * cos_b[...] - sin_at * sin_b[...]
        features[waves:, here] = sin_at * cos_b[...] + cos_at * sin_b[...]
    one = (lax.broadcasted_iota(jnp.int32, (pad, PERIOD), 0) == 0).astype(F32)

    def dense(weight, bias, value):
        layer[...] = jnp.zeros_like(layer)
        layer[:width, :width] = weight[...]
        layer[width : width + 1, :width] = bias[...]
        turned = layer[...].T[:width, : width + pad]
        return jnp.maximum(dot3(split(turned), split(jnp.concatenate([value, one], axis=0))), 0.0)

    hidden = dense(in_w, in_b, features[...])
    hidden = dense(mid_w, mid_b, hidden)
    per_tile = lanes // chans
    tile = out_w[:, pl.ds(pl.multiple_of(me // per_tile * lanes, lanes), lanes)]
    own = pltpu.roll(tile, lanes - me % per_tile * chans, 1).T[:pad, :]
    lines = dot3(split(own), split(hidden))
    for at in range(near):
        shapes[at * pad : (at + 1) * pad, :] = lines[:, at * lanes : (at + 1) * lanes]
    spots = (
        lax.broadcasted_iota(jnp.int32, (near, lanes), 0) * lanes
        + lax.broadcasted_iota(jnp.int32, (near, lanes), 1)
    ).astype(F32) / seq_length
    kernels = []
    for chan in range(chans):
        rate = jnp.full((near, lanes), decay[me * chans + chan], F32)
        envelope = jnp.exp(-rate * spots) * jnp.sqrt(2.0 * rate / seq_length)
        kernels.append(shapes[pl.ds(chan, near, stride=pad), :] * envelope)
    grid = jnp.concatenate(kernels, axis=1)
    forms = dot3((first[:, :near], first_low[:, :near]), split(grid))
    rows = []
    for chan in range(chans):
        here = slice(chan * lanes, (chan + 1) * lanes)
        real, imag = forms[:outer, here], forms[outer:, here]
        rows.append(
            jnp.concatenate(
                [real * turn[0] - imag * turn[1], real * turn[1] + imag * turn[0]], axis=1
            )
        )
    spec = dot3(split(jnp.concatenate(rows, axis=0)), (second[...], second_low[...]))
    scale = 1.0 / (outer * lanes)
    spec_real[...] = spec[:, :lanes] * scale
    spec_imag[...] = spec[:, lanes:] * scale


def convolve_kernel(
    values, spec_real, spec_imag, decay, first, first_low, second, second_low, back, back_low, last, last_low, turn,
    out, *, ratio
):
    outer, lanes = turn.shape[1], turn.shape[2]
    near = outer // 2
    chans = spec_real.shape[0] // outer
    peers = values.shape[0] // chans
    blocks = peers // near
    pairs = blocks // 2
    columns = []
    for chan in range(chans):
        lines = values[pl.ds(chan, peers, stride=chans), :]
        rate = jnp.full((1, lanes), decay[lax.axis_index("seq") * chans + chan], F32)
        keep = jnp.exp(-rate * ratio)
        carried = [jnp.zeros((near, lanes), F32), lines[:near]]
        for block in range(1, blocks):
            carried.append(lines[block * near : (block + 1) * near] + keep * carried[-1])
        for pair in range(pairs):
            low = 2 * pair
            columns.append(
                jnp.concatenate(
                    [carried[low], carried[low + 1], carried[low + 1], carried[low + 2]], axis=0
                )
            )
    forms = dot3((first[...], first_low[...]), split(jnp.concatenate(columns, axis=1)))
    turn_real, turn_imag = turn[0], turn[1]
    rows = []
    for at in range(chans * pairs):
        here = slice(at * lanes, (at + 1) * lanes)
        real, imag = forms[:outer, here], forms[outer:, here]
        rows.append(
            jnp.concatenate(
                [real * turn_real - imag * turn_imag, real * turn_imag + imag * turn_real], axis=1
            )
        )
    spec = dot3(split(jnp.concatenate(rows, axis=0)), (second[...], second_low[...]))
    rows = []
    for at in range(chans * pairs):
        chan = at // pairs
        real = spec[at * outer : (at + 1) * outer, :lanes]
        imag = spec[at * outer : (at + 1) * outer, lanes:]
        k_real = spec_real[chan * outer : (chan + 1) * outer, :]
        k_imag = spec_imag[chan * outer : (chan + 1) * outer, :]
        rows.append(
            jnp.concatenate(
                [real * k_real - imag * k_imag, real * k_imag + imag * k_real], axis=1
            )
        )
    forms = dot3(split(jnp.concatenate(rows, axis=0)), (back[...], back_low[...]))
    columns = []
    for at in range(chans * pairs):
        real = forms[at * outer : (at + 1) * outer, :lanes]
        imag = forms[at * outer : (at + 1) * outer, lanes:]
        columns.append(
            jnp.concatenate(
                [real * turn_real + imag * turn_imag, imag * turn_real - real * turn_imag], axis=0
            )
        )
    lines = dot3((last[...], last_low[...]), split(jnp.concatenate(columns, axis=1)))
    for chan in range(chans):
        both = [
            lines[:, (chan * pairs + pair) * lanes : (chan * pairs + pair + 1) * lanes]
            for pair in range(pairs)
        ]
        out[pl.ds(chan, peers, stride=chans), :] = jnp.concatenate(both, axis=0)


def prepare_kernel(
    tokens, gate_w, value_w, out_w,
    value_sum, gate_sum, value_high, value_low, gate_high, gate_low, send_high, send_low, keep_high, keep_low
):
    width = tokens.shape[1]
    me = lax.axis_index("chan")
    mine = pl.ds(pl.multiple_of(me * width, width), width)
    other = pl.ds(pl.multiple_of((1 - me) * width, width), width)
    own = split(tokens[...])
    value_sum[...] = dot3(own, split(value_w[mine, :]))
    gate_sum[...] = dot3(own, split(gate_w[mine, :]))
    value_high[...], value_low[...] = split(value_w[other, :])
    gate_high[...], gate_low[...] = split(gate_w[other, :])
    send_high[...], send_low[...] = split(out_w[:, other])
    keep_high[...], keep_low[...] = split(out_w[:, mine])


def project_kernel(tokens, value_in, gate_in, value_high, value_low, gate_high, gate_low, values, gated):
    terms = split(tokens[...])
    values[...] = silu(value_in[...] + dot3(terms, (value_high[...], value_low[...]))).T
    gated[...] = silu(gate_in[...] + dot3(terms, (gate_high[...], gate_low[...])))


def send_kernel(conv, gated, w_high, w_low, out, term_high, term_low):
    terms = split(gated[...] * conv[...].T)
    term_high[...], term_low[...] = terms
    out[...] = dot3(terms, (w_high[...], w_low[...]))


def keep_kernel(term_high, term_low, w_high, w_low, out):
    out[...] = dot3((term_high[...], term_low[...]), (w_high[...], w_low[...]))


def angle_tables(steps, wave_numbers):
    phases = wave_numbers[:, None] * steps[None, :] % PERIOD
    angles = phases.astype(F32) * (2.0 * math.pi / PERIOD)
    return jnp.cos(angles), jnp.sin(angles)


def on_device(
    tokens,
    gate_weight,
    value_weight,
    output_weight,
    wave_numbers,
    position_in,
    bias_in,
    position_mid,
    bias_mid,
    position_out,
    decay_rate,
):
    peer_count = lax.axis_size("seq")
    row_count, local_width = tokens.shape
    seq_length = row_count * peer_count
    chans = local_width // peer_count
    near = PERIOD // row_count
    outer = 2 * near
    swap = [(0, 1), (1, 0)]
    other_tokens = lax.ppermute(tokens, "chan", swap)

    first, second, last, turn = fourier_tables(outer, row_count)
    first_h, first_l = split_table(first)
    second_h, second_l = split_table(second)
    back_h, back_l = split_table(second.T)
    last_h, last_l = split_table(last)

    cos_a, sin_a = angle_tables(jnp.arange(near, dtype=jnp.int32) * row_count, wave_numbers)
    cos_b, sin_b = angle_tables(jnp.arange(row_count, dtype=jnp.int32), wave_numbers)

    def shaped(*dims, dtype=F32):
        return jax.ShapeDtypeStruct(dims, dtype)

    width = position_in.shape[0]
    spec_real, spec_imag = call(
        lambda *refs: spectrum_kernel(*refs, seq_length=seq_length),
        [shaped(chans * outer, row_count)] * 2,
        [
            pltpu.VMEM((width, PERIOD), F32),
            pltpu.VMEM((8 * near, row_count), F32),
            pltpu.VMEM((row_count, row_count), F32),
        ],
        10**9,
        scalars={9},
        name="spectrum",
    )(
        cos_a, sin_a, cos_b, sin_b, position_in, bias_in[None, :], position_mid, bias_mid[None, :], position_out,
        decay_rate, first_h, first_l, second_h, second_l, turn,
    )
    block = shaped(local_width, local_width, dtype=BF16)
    rows = shaped(row_count, local_width)
    prepared = call(prepare_kernel, [rows, rows] + [block] * 8, flops=10**9, name="prepare")(
        tokens, gate_weight, value_weight, output_weight
    )
    other_tokens, spec_real, spec_imag, prepared = lax.optimization_barrier(
        (other_tokens, spec_real, spec_imag, prepared)
    )
    (
        value_sum, gate_sum, value_high, value_low, gate_high, gate_low, send_high, send_low, keep_high, keep_low,
    ) = prepared
    weights = (value_high, value_low, gate_high, gate_low)
    flat = shaped(local_width, row_count)
    values, gated = call(project_kernel, [flat, rows], flops=10**8, name="project")(
        other_tokens, value_sum, gate_sum, *weights
    )
    value_lines = lax.all_to_all(values, "seq", split_axis=0, concat_axis=0, tiled=True)
    conv_lines = call(
        lambda *refs: convolve_kernel(*refs, ratio=PERIOD / seq_length), flat, flops=10**9, scalars={3},
        name="convolve",
    )(
        value_lines, spec_real, spec_imag, decay_rate, first_h, first_l, second_h, second_l, back_h, back_l,
        last_h, last_l, turn,
    )
    conv = lax.all_to_all(conv_lines, "seq", split_axis=0, concat_axis=0, tiled=True)
    term = shaped(row_count, local_width, dtype=BF16)
    sent, term_high, term_low = call(send_kernel, [rows, term, term], flops=10**8, name="send")(
        conv, gated, send_high, send_low
    )
    received = lax.ppermute(sent, "chan", swap)
    kept = call(keep_kernel, rows, flops=10**8, name="keep")(term_high, term_low, keep_high, keep_low)
    return kept + received


def solution(mesh):
    placed = (
        P("seq", "chan"),
        P(None, "chan"),
        P(None, "chan"),
        P("chan", None),
        P(),
        P(),
        P(),
        P(),
        P(),
        P(None, "chan"),
        P("chan"),
    )
    return jax.shard_map(
        on_device, mesh=mesh, in_specs=placed, out_specs=P("seq", "chan"), check_vma=False
    )
```

```python
import math

import jax
import jax.numpy as jnp
import numpy as np
from jax import lax
from jax.experimental import pallas as pl
from jax.experimental.pallas import tpu as pltpu
from jax.sharding import PartitionSpec as P

PERIOD = 4096
CORES = 2
F32 = jnp.float32
BF16 = jnp.bfloat16


def split(value):
    high = value.astype(BF16)
    low = (value - high.astype(F32)).astype(BF16)
    return high, low


def split_table(table):
    high = table.astype(np.float32).astype(jnp.bfloat16)
    low = (table - high.astype(np.float64)).astype(np.float32).astype(jnp.bfloat16)
    return high, low


def matmul(left, right):
    return jnp.dot(left, right, preferred_element_type=F32)


def dot3(left, right):
    left_high, left_low = left
    right_high, right_low = right
    return (
        matmul(left_high, right_low)
        + matmul(left_low, right_high)
        + matmul(left_high, right_high)
    )


def silu(value):
    return value / (1.0 + jnp.exp(-value))


def fourier_tables(outer, inner):
    n1 = np.arange(outer)
    n2 = np.arange(inner)
    angle = 2.0 * np.pi * ((n1[:, None] * n1[None, :]) % outer) / outer
    cos1, sin1 = np.cos(angle), np.sin(angle)
    first = np.block([[cos1, sin1], [-sin1, cos1]])
    half = outer // 2
    last = np.block([[cos1[half:], -sin1[half:]], [sin1[half:], cos1[half:]]])
    angle = 2.0 * np.pi * ((n2[:, None] * n2[None, :]) % inner) / inner
    cos2, sin2 = np.cos(angle), np.sin(angle)
    second = np.block([[cos2, -sin2], [sin2, cos2]])
    angle = 2.0 * np.pi * (n1[:, None] * n2[None, :]) / (outer * inner)
    turn = np.stack([np.cos(angle), -np.sin(angle)]).astype(np.float32)
    return first, second, last, turn


def call(kernel, out_shapes, scratch=(), flops=0, scalars=(), aliases=None, *, name):
    vmem = pl.BlockSpec(memory_space=pltpu.VMEM)
    smem = pl.BlockSpec(memory_space=pltpu.SMEM)
    many = isinstance(out_shapes, (list, tuple))

    def run(*args):
        return pl.pallas_call(
            kernel,
            out_shape=out_shapes,
            in_specs=[smem if at in scalars else vmem for at in range(len(args))],
            out_specs=[vmem] * len(out_shapes) if many else vmem,
            scratch_shapes=list(scratch),
            name=name,
            input_output_aliases=aliases or {},
            compiler_params=pltpu.CompilerParams(vmem_limit_bytes=48 << 20),
            cost_estimate=pl.CostEstimate(flops=flops, transcendentals=0, bytes_accessed=0),
        )(*args)

    return run


def core_index():
    return lax.axis_index("seq") % CORES


def first_channel(width, chans):
    return core_index() * (width // CORES) + lax.axis_index("seq") // CORES * chans


def spectrum_kernel(
    cos_a, sin_a, cos_b, sin_b, in_w, in_b, mid_w, mid_b, out_w, decay, first, first_low, second, second_low, turn,
    spec_real, spec_imag, features, shapes, layer, *, seq_length
):
    near, lanes = cos_a.shape[1], cos_b.shape[1]
    waves, width = cos_a.shape[0], in_w.shape[0]
    outer = turn.shape[1]
    chans = spec_real.shape[0] // outer
    own_first = first_channel(out_w.shape[1], chans)
    pad = 8
    for at in range(near):
        here = slice(at * lanes, (at + 1) * lanes)
        cos_at, sin_at = cos_a[:, at : at + 1], sin_a[:, at : at + 1]
        features[:waves, here] = cos_at * cos_b[...] - sin_at * sin_b[...]
        features[waves:, here] = sin_at * cos_b[...] + cos_at * sin_b[...]
    one = (lax.broadcasted_iota(jnp.int32, (pad, PERIOD), 0) == 0).astype(F32)

    def dense(weight, bias, value):
        layer[...] = jnp.zeros_like(layer)
        layer[:width, :width] = weight[...]
        layer[width : width + 1, :width] = bias[...]
        turned = layer[...].T[:width, : width + pad]
        return jnp.maximum(dot3(split(turned), split(jnp.concatenate([value, one], axis=0))), 0.0)

    hidden = dense(in_w, in_b, features[...])
    hidden = dense(mid_w, mid_b, hidden)
    tile = out_w[:, pl.ds(pl.multiple_of(own_first // lanes * lanes, lanes), lanes)]
    own = pltpu.roll(tile, lanes - own_first % lanes, 1).T[:pad, :]
    lines = dot3(split(own), split(hidden))
    for at in range(near):
        shapes[at * pad : (at + 1) * pad, :] = lines[:, at * lanes : (at + 1) * lanes]
    spots = (
        lax.broadcasted_iota(jnp.int32, (near, lanes), 0) * lanes
        + lax.broadcasted_iota(jnp.int32, (near, lanes), 1)
    ).astype(F32) / seq_length
    kernels = []
    for chan in range(chans):
        rate = jnp.full((near, lanes), decay[own_first + chan], F32)
        envelope = jnp.exp(-rate * spots) * jnp.sqrt(2.0 * rate / seq_length)
        kernels.append(shapes[pl.ds(chan, near, stride=pad), :] * envelope)
    grid = jnp.concatenate(kernels, axis=1)
    forms = dot3((first[:, :near], first_low[:, :near]), split(grid))
    rows = []
    for chan in range(chans):
        here = slice(chan * lanes, (chan + 1) * lanes)
        real, imag = forms[:outer, here], forms[outer:, here]
        rows.append(
            jnp.concatenate(
                [real * turn[0] - imag * turn[1], real * turn[1] + imag * turn[0]], axis=1
            )
        )
    spec = dot3(split(jnp.concatenate(rows, axis=0)), (second[...], second_low[...]))
    scale = 1.0 / (outer * lanes)
    spec_real[...] = spec[:, :lanes] * scale
    spec_imag[...] = spec[:, lanes:] * scale


def convolve_kernel(
    values, spec_real, spec_imag, decay, first, first_low, second, second_low, back, back_low, last, last_low, turn,
    out, *, ratio
):
    outer, lanes = turn.shape[1], turn.shape[2]
    near = outer // 2
    chans = spec_real.shape[0] // outer
    peers = values.shape[0] // chans
    blocks = peers // near
    pairs = blocks // 2
    columns = []
    for chan in range(chans):
        lines = values[pl.ds(chan, peers, stride=chans), :]
        rate = jnp.full((1, lanes), decay[first_channel(decay.shape[0], chans) + chan], F32)
        keep = jnp.exp(-rate * ratio)
        carried = [jnp.zeros((near, lanes), F32), lines[:near]]
        for block in range(1, blocks):
            carried.append(lines[block * near : (block + 1) * near] + keep * carried[-1])
        for pair in range(pairs):
            low = 2 * pair
            columns.append(
                jnp.concatenate(
                    [carried[low], carried[low + 1], carried[low + 1], carried[low + 2]], axis=0
                )
            )
    forms = dot3((first[...], first_low[...]), split(jnp.concatenate(columns, axis=1)))
    turn_real, turn_imag = turn[0], turn[1]
    rows = []
    for at in range(chans * pairs):
        here = slice(at * lanes, (at + 1) * lanes)
        real, imag = forms[:outer, here], forms[outer:, here]
        rows.append(
            jnp.concatenate(
                [real * turn_real - imag * turn_imag, real * turn_imag + imag * turn_real], axis=1
            )
        )
    spec = dot3(split(jnp.concatenate(rows, axis=0)), (second[...], second_low[...]))
    rows = []
    for at in range(chans * pairs):
        chan = at // pairs
        real = spec[at * outer : (at + 1) * outer, :lanes]
        imag = spec[at * outer : (at + 1) * outer, lanes:]
        k_real = spec_real[chan * outer : (chan + 1) * outer, :]
        k_imag = spec_imag[chan * outer : (chan + 1) * outer, :]
        rows.append(
            jnp.concatenate(
                [real * k_real - imag * k_imag, real * k_imag + imag * k_real], axis=1
            )
        )
    forms = dot3(split(jnp.concatenate(rows, axis=0)), (back[...], back_low[...]))
    columns = []
    for at in range(chans * pairs):
        real = forms[at * outer : (at + 1) * outer, :lanes]
        imag = forms[at * outer : (at + 1) * outer, lanes:]
        columns.append(
            jnp.concatenate(
                [real * turn_real + imag * turn_imag, imag * turn_real - real * turn_imag], axis=0
            )
        )
    lines = dot3((last[...], last_low[...]), split(jnp.concatenate(columns, axis=1)))
    for chan in range(chans):
        both = [
            lines[:, (chan * pairs + pair) * lanes : (chan * pairs + pair + 1) * lanes]
            for pair in range(pairs)
        ]
        out[pl.ds(chan, peers, stride=chans), :] = jnp.concatenate(both, axis=0)


def prepare_kernel(
    tokens, gate_w, value_w, out_w,
    value_sum, gate_sum, value_high, value_low, gate_high, gate_low, send_high, send_low, keep_high, keep_low
):
    width = tokens.shape[1]
    half = width // CORES
    me, core = lax.axis_index("chan"), core_index()
    mine = pl.ds(pl.multiple_of(me * width, width), width)
    other = pl.ds(pl.multiple_of((1 - me) * width, width), width)
    own = split(tokens[...])
    for at, part in ((0, core), (half, 1 - core)):
        here, there = slice(at, at + half), pl.ds(pl.multiple_of(part * half, half), half)
        value_sum[:, here] = dot3(own, split(value_w[mine, there]))
        gate_sum[:, here] = dot3(own, split(gate_w[mine, there]))
        value_high[:, here], value_low[:, here] = split(value_w[other, there])
        gate_high[:, here], gate_low[:, here] = split(gate_w[other, there])
        send_high[here, :], send_low[here, :] = split(out_w[there, other])
        keep_high[here, :], keep_low[here, :] = split(out_w[there, mine])


def sibling_kernel(tokens, value_in, value_high, value_low, sibling):
    half = sibling.shape[0]
    terms = split(tokens[...])
    values = value_in[:, half:] + dot3(terms, (value_high[:, half:], value_low[:, half:]))
    sibling[...] = silu(values).T


def mine_kernel(tokens, value_in, gate_in, value_high, value_low, gate_high, gate_low, merged, gated, mine, *, chans):
    half = mine.shape[0]
    terms = split(tokens[...])
    values = value_in[:, :half] + dot3(terms, (value_high[:, :half], value_low[:, :half]))
    mine[...] = silu(values).T
    gated[...] = silu(gate_in[...] + dot3(terms, (gate_high[...], gate_low[...])))
    interleave(mine, merged, core_index(), chans)


def interleave(part, merged, core, chans):
    count = part.shape[0] // chans
    for chan in range(chans):
        rows = part[pl.ds(chan, count, stride=chans), :]
        merged[pl.ds(core * chans + chan, count, stride=CORES * chans), :] = rows


def extract(merged, part, core, chans):
    count = part.shape[0] // chans
    for chan in range(chans):
        rows = merged[pl.ds(core * chans + chan, count, stride=CORES * chans), :]
        part[pl.ds(chan, count, stride=chans), :] = rows


def merge_kernel(part, _, merged, *, chans):
    interleave(part, merged, 1 - core_index(), chans)


def extract_kernel(merged, part, *, chans):
    extract(merged, part, 1 - core_index(), chans)


def first_kernel(merged, gated, send_high, send_low, keep_high, keep_low, sent, kept, mine, *, chans):
    half = mine.shape[0]
    extract(merged, mine, core_index(), chans)
    terms = split(gated[:, :half] * mine[...].T)
    sent[...] = dot3(terms, (send_high[:half, :], send_low[:half, :]))
    kept[...] = dot3(terms, (keep_high[:half, :], keep_low[:half, :]))


def send_kernel(conv, gated, part, w_high, w_low, out, term_high, term_low):
    half = conv.shape[0]
    terms = split(gated[:, half:] * conv[...].T)
    term_high[...], term_low[...] = terms
    out[...] = part[...] + dot3(terms, (w_high[half:, :], w_low[half:, :]))


def keep_kernel(term_high, term_low, part, w_high, w_low, out):
    half = term_high.shape[1]
    out[...] = part[...] + dot3((term_high[...], term_low[...]), (w_high[half:, :], w_low[half:, :]))


def angle_tables(steps, wave_numbers):
    phases = wave_numbers[:, None] * steps[None, :] % PERIOD
    angles = phases.astype(F32) * (2.0 * math.pi / PERIOD)
    return jnp.cos(angles), jnp.sin(angles)


def on_device(
    tokens,
    gate_weight,
    value_weight,
    output_weight,
    wave_numbers,
    position_in,
    bias_in,
    position_mid,
    bias_mid,
    position_out,
    decay_rate,
):
    peer_count = lax.axis_size("seq")
    row_count, local_width = tokens.shape
    seq_length = row_count * peer_count
    chans = local_width // peer_count
    near = PERIOD // row_count
    outer = 2 * near
    swap = [(0, 1), (1, 0)]
    other_tokens = lax.ppermute(tokens, "chan", swap)

    first, second, last, turn = fourier_tables(outer, row_count)
    first_h, first_l = split_table(first)
    second_h, second_l = split_table(second)
    back_h, back_l = split_table(second.T)
    last_h, last_l = split_table(last)

    cos_a, sin_a = angle_tables(jnp.arange(near, dtype=jnp.int32) * row_count, wave_numbers)
    cos_b, sin_b = angle_tables(jnp.arange(row_count, dtype=jnp.int32), wave_numbers)

    def shaped(*dims, dtype=F32):
        return jax.ShapeDtypeStruct(dims, dtype)

    width = position_in.shape[0]
    spec_real, spec_imag = call(
        lambda *refs: spectrum_kernel(*refs, seq_length=seq_length),
        [shaped(chans * outer, row_count)] * 2,
        [
            pltpu.VMEM((width, PERIOD), F32),
            pltpu.VMEM((8 * near, row_count), F32),
            pltpu.VMEM((row_count, row_count), F32),
        ],
        10**9,
        scalars={9},
        name="spectrum",
    )(
        cos_a, sin_a, cos_b, sin_b, position_in, bias_in[None, :], position_mid, bias_mid[None, :], position_out,
        decay_rate, first_h, first_l, second_h, second_l, turn,
    )
    block = shaped(local_width, local_width, dtype=BF16)
    rows = shaped(row_count, local_width)
    prepared = call(prepare_kernel, [rows, rows] + [block] * 8, flops=10**9, name="prepare")(
        tokens, gate_weight, value_weight, output_weight
    )
    other_tokens, spec_real, spec_imag, prepared = lax.optimization_barrier(
        (other_tokens, spec_real, spec_imag, prepared)
    )
    (
        value_sum, gate_sum, value_high, value_low, gate_high, gate_low, send_high, send_low, keep_high, keep_low,
    ) = prepared
    weights = (value_high, value_low, gate_high, gate_low)
    flat = shaped(local_width, row_count)
    half = shaped(local_width // CORES, row_count)
    siblings = [(peer, peer ^ 1) for peer in range(peer_count)]
    same_core = [list(range(core, peer_count, CORES)) for core in range(CORES)]

    def with_chans(kernel):
        return lambda *refs: kernel(*refs, chans=chans)

    sibling = call(sibling_kernel, half, flops=10**8, name="sibling")(
        other_tokens, value_sum, value_high, value_low
    )
    sibling = lax.ppermute(sibling, "seq", siblings)
    merged, gated = call(
        with_chans(mine_kernel), [flat, rows], [pltpu.VMEM(half.shape, F32)], flops=10**8, name="mine"
    )(other_tokens, value_sum, gate_sum, *weights)
    merged = call(with_chans(merge_kernel), flat, aliases={1: 0}, name="merge")(sibling, merged)
    value_lines = lax.all_to_all(
        merged, "seq", split_axis=0, concat_axis=0, tiled=True, axis_index_groups=same_core
    )
    conv_lines = call(
        lambda *refs: convolve_kernel(*refs, ratio=PERIOD / seq_length), flat, flops=10**9, scalars={3},
        name="convolve",
    )(
        value_lines, spec_real, spec_imag, decay_rate, first_h, first_l, second_h, second_l, back_h, back_l,
        last_h, last_l, turn,
    )
    conv = lax.all_to_all(
        conv_lines, "seq", split_axis=0, concat_axis=0, tiled=True, axis_index_groups=same_core
    )
    sibling = call(with_chans(extract_kernel), half, name="extract")(conv)
    sibling = lax.ppermute(sibling, "seq", siblings)
    sent, kept = call(
        with_chans(first_kernel), [rows, rows], [pltpu.VMEM(half.shape, F32)], flops=10**8, name="first"
    )(conv, gated, send_high, send_low, keep_high, keep_low)
    term = shaped(row_count, local_width // CORES, dtype=BF16)
    sent, term_high, term_low = call(send_kernel, [rows, term, term], flops=10**8, name="send")(
        sibling, gated, sent, send_high, send_low
    )
    received = lax.ppermute(sent, "chan", swap)
    kept = call(keep_kernel, rows, flops=10**8, name="keep")(term_high, term_low, kept, keep_high, keep_low)
    return kept + received


def solution(mesh):
    placed = (
        P("seq", "chan"),
        P(None, "chan"),
        P(None, "chan"),
        P("chan", None),
        P(),
        P(),
        P(),
        P(),
        P(),
        P(None, "chan"),
        P("chan"),
    )
    return jax.shard_map(
        on_device, mesh=mesh, in_specs=placed, out_specs=P("seq", "chan"), check_vma=False
    )
```

```python
import math

import jax
import jax.numpy as jnp
import numpy as np
from jax import lax
from jax.experimental import pallas as pl
from jax.experimental.pallas import tpu as pltpu
from jax.sharding import PartitionSpec as P

PERIOD = 4096
CORES = 2
CHIP_ORDER = (
    8, 57, 27, 20, 33, 32, 29, 30, 62, 11, 26, 28, 1, 16, 0, 12,
    4, 10, 3, 21, 40, 25, 59, 9, 7, 6, 38, 31, 45, 56, 13, 19,
    44, 53, 52, 18, 41, 24, 17, 2, 22, 47, 50, 46, 49, 23, 34, 61,
    5, 39, 60, 37, 36, 15, 58, 43, 48, 51, 55, 42, 63, 35, 54, 14,
)
F32 = jnp.float32
BF16 = jnp.bfloat16


def split(value):
    high = value.astype(BF16)
    low = (value - high.astype(F32)).astype(BF16)
    return high, low


def split_table(table):
    high = table.astype(np.float32).astype(jnp.bfloat16)
    low = (table - high.astype(np.float64)).astype(np.float32).astype(jnp.bfloat16)
    return high, low


def matmul(left, right):
    return jnp.dot(left, right, preferred_element_type=F32)


def dot3(left, right):
    left_high, left_low = left
    right_high, right_low = right
    return (
        matmul(left_high, right_low)
        + matmul(left_low, right_high)
        + matmul(left_high, right_high)
    )


def silu(value):
    return value / (1.0 + jnp.exp(-value))


def fourier_tables(outer, inner):
    n1 = np.arange(outer)
    n2 = np.arange(inner)
    angle = 2.0 * np.pi * ((n1[:, None] * n1[None, :]) % outer) / outer
    cos1, sin1 = np.cos(angle), np.sin(angle)
    first = np.block([[cos1, sin1], [-sin1, cos1]])
    half = outer // 2
    last = np.block([[cos1[half:], -sin1[half:]], [sin1[half:], cos1[half:]]])
    angle = 2.0 * np.pi * ((n2[:, None] * n2[None, :]) % inner) / inner
    cos2, sin2 = np.cos(angle), np.sin(angle)
    second = np.block([[cos2, -sin2], [sin2, cos2]])
    angle = 2.0 * np.pi * (n1[:, None] * n2[None, :]) / (outer * inner)
    turn = np.stack([np.cos(angle), -np.sin(angle)]).astype(np.float32)
    return first, second, last, turn


def call(kernel, out_shapes, scratch=(), flops=0, scalars=(), aliases=None, *, name):
    vmem = pl.BlockSpec(memory_space=pltpu.VMEM)
    smem = pl.BlockSpec(memory_space=pltpu.SMEM)
    many = isinstance(out_shapes, (list, tuple))

    def run(*args):
        return pl.pallas_call(
            kernel,
            out_shape=out_shapes,
            in_specs=[smem if at in scalars else vmem for at in range(len(args))],
            out_specs=[vmem] * len(out_shapes) if many else vmem,
            scratch_shapes=list(scratch),
            name=name,
            input_output_aliases=aliases or {},
            compiler_params=pltpu.CompilerParams(vmem_limit_bytes=48 << 20),
            cost_estimate=pl.CostEstimate(flops=flops, transcendentals=0, bytes_accessed=0),
        )(*args)

    return run


def core_index():
    return lax.axis_index("seq") % CORES


def spectrum_kernel(
    cos_a, sin_a, cos_b, sin_b, in_w, in_b, mid_w, mid_b, out_w, decay, own, first, first_low, second, second_low, turn,
    spec_real, spec_imag, features, shapes, layer, *, seq_length
):
    near, lanes = cos_a.shape[1], cos_b.shape[1]
    waves, width = cos_a.shape[0], in_w.shape[0]
    outer = turn.shape[1]
    chans = spec_real.shape[0] // outer
    own_first = own[0]
    pad = 8
    for at in range(near):
        here = slice(at * lanes, (at + 1) * lanes)
        cos_at, sin_at = cos_a[:, at : at + 1], sin_a[:, at : at + 1]
        features[:waves, here] = cos_at * cos_b[...] - sin_at * sin_b[...]
        features[waves:, here] = sin_at * cos_b[...] + cos_at * sin_b[...]
    one = (lax.broadcasted_iota(jnp.int32, (pad, PERIOD), 0) == 0).astype(F32)

    def dense(weight, bias, value):
        layer[...] = jnp.zeros_like(layer)
        layer[:width, :width] = weight[...]
        layer[width : width + 1, :width] = bias[...]
        turned = layer[...].T[:width, : width + pad]
        return jnp.maximum(dot3(split(turned), split(jnp.concatenate([value, one], axis=0))), 0.0)

    hidden = dense(in_w, in_b, features[...])
    hidden = dense(mid_w, mid_b, hidden)
    tile = out_w[:, pl.ds(pl.multiple_of(own_first // lanes * lanes, lanes), lanes)]
    own_w = pltpu.roll(tile, lanes - own_first % lanes, 1).T[:pad, :]
    lines = dot3(split(own_w), split(hidden))
    for at in range(near):
        shapes[at * pad : (at + 1) * pad, :] = lines[:, at * lanes : (at + 1) * lanes]
    spots = (
        lax.broadcasted_iota(jnp.int32, (near, lanes), 0) * lanes
        + lax.broadcasted_iota(jnp.int32, (near, lanes), 1)
    ).astype(F32) / seq_length
    kernels = []
    for chan in range(chans):
        rate = jnp.full((near, lanes), decay[own_first + chan], F32)
        envelope = jnp.exp(-rate * spots) * jnp.sqrt(2.0 * rate / seq_length)
        kernels.append(shapes[pl.ds(chan, near, stride=pad), :] * envelope)
    grid = jnp.concatenate(kernels, axis=1)
    forms = dot3((first[:, :near], first_low[:, :near]), split(grid))
    rows = []
    for chan in range(chans):
        here = slice(chan * lanes, (chan + 1) * lanes)
        real, imag = forms[:outer, here], forms[outer:, here]
        rows.append(
            jnp.concatenate(
                [real * turn[0] - imag * turn[1], real * turn[1] + imag * turn[0]], axis=1
            )
        )
    spec = dot3(split(jnp.concatenate(rows, axis=0)), (second[...], second_low[...]))
    scale = 1.0 / (outer * lanes)
    spec_real[...] = spec[:, :lanes] * scale
    spec_imag[...] = spec[:, lanes:] * scale


def convolve_kernel(
    values, spec_real, spec_imag, decay, own, first, first_low, second, second_low, back, back_low, last, last_low,
    turn, out, ordered, *, ratio
):
    outer, lanes = turn.shape[1], turn.shape[2]
    near = outer // 2
    chans = spec_real.shape[0] // outer
    peers = values.shape[0] // chans
    blocks = peers // near
    pairs = blocks // 2
    columns = []
    tile = CORES * chans
    for place, chip in enumerate(CHIP_ORDER):
        ordered[chip * tile : (chip + 1) * tile, :] = values[place * tile : (place + 1) * tile, :]
    for chan in range(chans):
        lines = ordered[pl.ds(chan, peers, stride=chans), :]
        rate = jnp.full((1, lanes), decay[own[0] + chan], F32)
        keep = jnp.exp(-rate * ratio)
        carried = [jnp.zeros((near, lanes), F32), lines[:near]]
        for block in range(1, blocks):
            carried.append(lines[block * near : (block + 1) * near] + keep * carried[-1])
        for pair in range(pairs):
            low = 2 * pair
            columns.append(
                jnp.concatenate(
                    [carried[low], carried[low + 1], carried[low + 1], carried[low + 2]], axis=0
                )
            )
    forms = dot3((first[...], first_low[...]), split(jnp.concatenate(columns, axis=1)))
    turn_real, turn_imag = turn[0], turn[1]
    rows = []
    for at in range(chans * pairs):
        here = slice(at * lanes, (at + 1) * lanes)
        real, imag = forms[:outer, here], forms[outer:, here]
        rows.append(
            jnp.concatenate(
                [real * turn_real - imag * turn_imag, real * turn_imag + imag * turn_real], axis=1
            )
        )
    spec = dot3(split(jnp.concatenate(rows, axis=0)), (second[...], second_low[...]))
    rows = []
    for at in range(chans * pairs):
        chan = at // pairs
        real = spec[at * outer : (at + 1) * outer, :lanes]
        imag = spec[at * outer : (at + 1) * outer, lanes:]
        k_real = spec_real[chan * outer : (chan + 1) * outer, :]
        k_imag = spec_imag[chan * outer : (chan + 1) * outer, :]
        rows.append(
            jnp.concatenate(
                [real * k_real - imag * k_imag, real * k_imag + imag * k_real], axis=1
            )
        )
    forms = dot3(split(jnp.concatenate(rows, axis=0)), (back[...], back_low[...]))
    columns = []
    for at in range(chans * pairs):
        real = forms[at * outer : (at + 1) * outer, :lanes]
        imag = forms[at * outer : (at + 1) * outer, lanes:]
        columns.append(
            jnp.concatenate(
                [real * turn_real + imag * turn_imag, imag * turn_real - real * turn_imag], axis=0
            )
        )
    lines = dot3((last[...], last_low[...]), split(jnp.concatenate(columns, axis=1)))
    for chan in range(chans):
        both = [
            lines[:, (chan * pairs + pair) * lanes : (chan * pairs + pair + 1) * lanes]
            for pair in range(pairs)
        ]
        ordered[pl.ds(chan, peers, stride=chans), :] = jnp.concatenate(both, axis=0)
    for place, chip in enumerate(CHIP_ORDER):
        out[place * tile : (place + 1) * tile, :] = ordered[chip * tile : (chip + 1) * tile, :]


def prepare_kernel(
    tokens, gate_w, value_w, out_w,
    value_sum, gate_sum, value_high, value_low, gate_high, gate_low, send_high, send_low, keep_high, keep_low
):
    width = tokens.shape[1]
    half = width // CORES
    me, core = lax.axis_index("chan"), core_index()
    mine = pl.ds(pl.multiple_of(me * width, width), width)
    other = pl.ds(pl.multiple_of((1 - me) * width, width), width)
    own = split(tokens[...])
    for at, part in ((0, core), (half, 1 - core)):
        here, there = slice(at, at + half), pl.ds(pl.multiple_of(part * half, half), half)
        value_sum[:, here] = dot3(own, split(value_w[mine, there]))
        gate_sum[:, here] = dot3(own, split(gate_w[mine, there]))
        value_high[:, here], value_low[:, here] = split(value_w[other, there])
        gate_high[:, here], gate_low[:, here] = split(gate_w[other, there])
        send_high[here, :], send_low[here, :] = split(out_w[there, other])
        keep_high[here, :], keep_low[here, :] = split(out_w[there, mine])


def sibling_kernel(tokens, value_in, value_high, value_low, sibling):
    half = sibling.shape[0]
    terms = split(tokens[...])
    values = value_in[:, half:] + dot3(terms, (value_high[:, half:], value_low[:, half:]))
    sibling[...] = silu(values).T


def mine_kernel(tokens, value_in, gate_in, value_high, value_low, gate_high, gate_low, merged, gated, mine, *, chans):
    half = mine.shape[0]
    terms = split(tokens[...])
    values = value_in[:, :half] + dot3(terms, (value_high[:, :half], value_low[:, :half]))
    mine[...] = silu(values).T
    gated[...] = silu(gate_in[...] + dot3(terms, (gate_high[...], gate_low[...])))
    interleave(mine, merged, core_index(), chans)


def interleave(part, merged, core, chans):
    count = part.shape[0] // chans
    for chan in range(chans):
        rows = part[pl.ds(chan, count, stride=chans), :]
        merged[pl.ds(core * chans + chan, count, stride=CORES * chans), :] = rows


def extract(merged, part, core, chans):
    count = part.shape[0] // chans
    for chan in range(chans):
        rows = merged[pl.ds(core * chans + chan, count, stride=CORES * chans), :]
        part[pl.ds(chan, count, stride=chans), :] = rows


def merge_kernel(part, _, merged, *, chans):
    interleave(part, merged, 1 - core_index(), chans)


def extract_kernel(merged, part, *, chans):
    extract(merged, part, 1 - core_index(), chans)


def first_kernel(merged, gated, send_high, send_low, keep_high, keep_low, sent, kept, mine, *, chans):
    half = mine.shape[0]
    extract(merged, mine, core_index(), chans)
    terms = split(gated[:, :half] * mine[...].T)
    sent[...] = dot3(terms, (send_high[:half, :], send_low[:half, :]))
    kept[...] = dot3(terms, (keep_high[:half, :], keep_low[:half, :]))


def send_kernel(conv, gated, part, w_high, w_low, out, term_high, term_low):
    half = conv.shape[0]
    terms = split(gated[:, half:] * conv[...].T)
    term_high[...], term_low[...] = terms
    out[...] = part[...] + dot3(terms, (w_high[half:, :], w_low[half:, :]))


def keep_kernel(term_high, term_low, part, w_high, w_low, out):
    half = term_high.shape[1]
    out[...] = part[...] + dot3((term_high[...], term_low[...]), (w_high[half:, :], w_low[half:, :]))


def angle_tables(steps, wave_numbers):
    phases = wave_numbers[:, None] * steps[None, :] % PERIOD
    angles = phases.astype(F32) * (2.0 * math.pi / PERIOD)
    return jnp.cos(angles), jnp.sin(angles)


def on_device(
    tokens,
    gate_weight,
    value_weight,
    output_weight,
    wave_numbers,
    position_in,
    bias_in,
    position_mid,
    bias_mid,
    position_out,
    decay_rate,
):
    peer_count = lax.axis_size("seq")
    row_count, local_width = tokens.shape
    seq_length = row_count * peer_count
    chans = local_width // peer_count
    near = PERIOD // row_count
    outer = 2 * near
    swap = [(0, 1), (1, 0)]
    other_tokens = lax.ppermute(tokens, "chan", swap)

    first, second, last, turn = fourier_tables(outer, row_count)
    first_h, first_l = split_table(first)
    second_h, second_l = split_table(second)
    back_h, back_l = split_table(second.T)
    last_h, last_l = split_table(last)

    me = lax.axis_index("seq")
    place_of = jnp.asarray(np.argsort(CHIP_ORDER).astype(np.int32))
    place = lax.dynamic_slice_in_dim(place_of, me // CORES, 1)
    own_first = me % CORES * (local_width // CORES) + place * chans
    cos_a, sin_a = angle_tables(jnp.arange(near, dtype=jnp.int32) * row_count, wave_numbers)
    cos_b, sin_b = angle_tables(jnp.arange(row_count, dtype=jnp.int32), wave_numbers)

    def shaped(*dims, dtype=F32):
        return jax.ShapeDtypeStruct(dims, dtype)

    width = position_in.shape[0]
    spec_real, spec_imag = call(
        lambda *refs: spectrum_kernel(*refs, seq_length=seq_length),
        [shaped(chans * outer, row_count)] * 2,
        [
            pltpu.VMEM((width, PERIOD), F32),
            pltpu.VMEM((8 * near, row_count), F32),
            pltpu.VMEM((row_count, row_count), F32),
        ],
        10**9,
        scalars={9, 10},
        name="spectrum",
    )(
        cos_a, sin_a, cos_b, sin_b, position_in, bias_in[None, :], position_mid, bias_mid[None, :], position_out,
        decay_rate, own_first, first_h, first_l, second_h, second_l, turn,
    )
    block = shaped(local_width, local_width, dtype=BF16)
    rows = shaped(row_count, local_width)
    prepared = call(prepare_kernel, [rows, rows] + [block] * 8, flops=10**9, name="prepare")(
        tokens, gate_weight, value_weight, output_weight
    )
    other_tokens, spec_real, spec_imag, prepared = lax.optimization_barrier(
        (other_tokens, spec_real, spec_imag, prepared)
    )
    (
        value_sum, gate_sum, value_high, value_low, gate_high, gate_low, send_high, send_low, keep_high, keep_low,
    ) = prepared
    weights = (value_high, value_low, gate_high, gate_low)
    flat = shaped(local_width, row_count)
    half = shaped(local_width // CORES, row_count)
    siblings = [(peer, peer ^ 1) for peer in range(peer_count)]
    same_core = [[CORES * chip + core for chip in CHIP_ORDER] for core in range(CORES)]

    def with_chans(kernel):
        return lambda *refs: kernel(*refs, chans=chans)

    sibling = call(sibling_kernel, half, flops=10**8, name="sibling")(
        other_tokens, value_sum, value_high, value_low
    )
    sibling = lax.ppermute(sibling, "seq", siblings)
    merged, gated = call(
        with_chans(mine_kernel), [flat, rows], [pltpu.VMEM(half.shape, F32)], flops=10**8, name="mine"
    )(other_tokens, value_sum, gate_sum, *weights)
    merged = call(with_chans(merge_kernel), flat, aliases={1: 0}, name="merge")(sibling, merged)
    value_lines = lax.all_to_all(
        merged, "seq", split_axis=0, concat_axis=0, tiled=True, axis_index_groups=same_core
    )
    conv_lines = call(
        lambda *refs: convolve_kernel(*refs, ratio=PERIOD / seq_length), flat, [pltpu.VMEM(flat.shape, F32)],
        flops=10**9, scalars={3, 4}, name="convolve",
    )(
        value_lines, spec_real, spec_imag, decay_rate, own_first, first_h, first_l, second_h, second_l, back_h, back_l,
        last_h, last_l, turn,
    )
    conv = lax.all_to_all(
        conv_lines, "seq", split_axis=0, concat_axis=0, tiled=True, axis_index_groups=same_core
    )
    sibling = call(with_chans(extract_kernel), half, name="extract")(conv)
    sibling = lax.ppermute(sibling, "seq", siblings)
    sent, kept = call(
        with_chans(first_kernel), [rows, rows], [pltpu.VMEM(half.shape, F32)], flops=10**8, name="first"
    )(conv, gated, send_high, send_low, keep_high, keep_low)
    term = shaped(row_count, local_width // CORES, dtype=BF16)
    sent, term_high, term_low = call(send_kernel, [rows, term, term], flops=10**8, name="send")(
        sibling, gated, sent, send_high, send_low
    )
    received = lax.ppermute(sent, "chan", swap)
    kept = call(keep_kernel, rows, flops=10**8, name="keep")(term_high, term_low, kept, keep_high, keep_low)
    return kept + received


def solution(mesh):
    placed = (
        P("seq", "chan"),
        P(None, "chan"),
        P(None, "chan"),
        P("chan", None),
        P(),
        P(),
        P(),
        P(),
        P(),
        P(None, "chan"),
        P("chan"),
    )
    return jax.shard_map(
        on_device, mesh=mesh, in_specs=placed, out_specs=P("seq", "chan"), check_vma=False
    )
```

```python
import math

import jax
import jax.numpy as jnp
import numpy as np
from jax import lax
from jax.experimental import pallas as pl
from jax.experimental.pallas import tpu as pltpu
from jax.sharding import PartitionSpec as P

PERIOD = 4096
CORES = 2
CHIP_ORDER = tuple((42 + place) % 64 for place in range(64))
F32 = jnp.float32
BF16 = jnp.bfloat16


def split(value):
    high = value.astype(BF16)
    low = (value - high.astype(F32)).astype(BF16)
    return high, low


def split_table(table):
    high = table.astype(np.float32).astype(jnp.bfloat16)
    low = (table - high.astype(np.float64)).astype(np.float32).astype(jnp.bfloat16)
    return high, low


def matmul(left, right):
    return jnp.dot(left, right, preferred_element_type=F32)


def dot3(left, right):
    left_high, left_low = left
    right_high, right_low = right
    return (
        matmul(left_high, right_low)
        + matmul(left_low, right_high)
        + matmul(left_high, right_high)
    )


def silu(value):
    return value / (1.0 + jnp.exp(-value))


def fourier_tables(outer, inner):
    n1 = np.arange(outer)
    n2 = np.arange(inner)
    angle = 2.0 * np.pi * ((n1[:, None] * n1[None, :]) % outer) / outer
    cos1, sin1 = np.cos(angle), np.sin(angle)
    first = np.block([[cos1, sin1], [-sin1, cos1]])
    half = outer // 2
    last = np.block([[cos1[half:], -sin1[half:]], [sin1[half:], cos1[half:]]])
    angle = 2.0 * np.pi * ((n2[:, None] * n2[None, :]) % inner) / inner
    cos2, sin2 = np.cos(angle), np.sin(angle)
    second = np.block([[cos2, -sin2], [sin2, cos2]])
    angle = 2.0 * np.pi * (n1[:, None] * n2[None, :]) / (outer * inner)
    turn = np.stack([np.cos(angle), -np.sin(angle)]).astype(np.float32)
    return first, second, last, turn


def call(kernel, out_shapes, scratch=(), flops=0, scalars=(), aliases=None, *, name):
    vmem = pl.BlockSpec(memory_space=pltpu.VMEM)
    smem = pl.BlockSpec(memory_space=pltpu.SMEM)
    many = isinstance(out_shapes, (list, tuple))

    def run(*args):
        return pl.pallas_call(
            kernel,
            out_shape=out_shapes,
            in_specs=[smem if at in scalars else vmem for at in range(len(args))],
            out_specs=[vmem] * len(out_shapes) if many else vmem,
            scratch_shapes=list(scratch),
            name=name,
            input_output_aliases=aliases or {},
            compiler_params=pltpu.CompilerParams(vmem_limit_bytes=48 << 20),
            cost_estimate=pl.CostEstimate(flops=flops, transcendentals=0, bytes_accessed=0),
        )(*args)

    return run


def core_index():
    return lax.axis_index("seq") % CORES


def spectrum_kernel(
    cos_a, sin_a, cos_b, sin_b, in_w, in_b, mid_w, mid_b, out_w, decay, own, first, first_low, second, second_low, turn,
    spec_real, spec_imag, features, shapes, layer, *, seq_length
):
    near, lanes = cos_a.shape[1], cos_b.shape[1]
    waves, width = cos_a.shape[0], in_w.shape[0]
    outer = turn.shape[1]
    chans = spec_real.shape[0] // outer
    own_first = own[0]
    pad = 8
    for at in range(near):
        here = slice(at * lanes, (at + 1) * lanes)
        cos_at, sin_at = cos_a[:, at : at + 1], sin_a[:, at : at + 1]
        features[:waves, here] = cos_at * cos_b[...] - sin_at * sin_b[...]
        features[waves:, here] = sin_at * cos_b[...] + cos_at * sin_b[...]
    one = (lax.broadcasted_iota(jnp.int32, (pad, PERIOD), 0) == 0).astype(F32)

    def dense(weight, bias, value):
        layer[...] = jnp.zeros_like(layer)
        layer[:width, :width] = weight[...]
        layer[width : width + 1, :width] = bias[...]
        turned = layer[...].T[:width, : width + pad]
        return jnp.maximum(dot3(split(turned), split(jnp.concatenate([value, one], axis=0))), 0.0)

    hidden = dense(in_w, in_b, features[...])
    hidden = dense(mid_w, mid_b, hidden)
    tile = out_w[:, pl.ds(pl.multiple_of(own_first // lanes * lanes, lanes), lanes)]
    own_w = pltpu.roll(tile, lanes - own_first % lanes, 1).T[:pad, :]
    lines = dot3(split(own_w), split(hidden))
    for at in range(near):
        shapes[at * pad : (at + 1) * pad, :] = lines[:, at * lanes : (at + 1) * lanes]
    spots = (
        lax.broadcasted_iota(jnp.int32, (near, lanes), 0) * lanes
        + lax.broadcasted_iota(jnp.int32, (near, lanes), 1)
    ).astype(F32) / seq_length
    kernels = []
    for chan in range(chans):
        rate = jnp.full((near, lanes), decay[own_first + chan], F32)
        envelope = jnp.exp(-rate * spots) * jnp.sqrt(2.0 * rate / seq_length)
        kernels.append(shapes[pl.ds(chan, near, stride=pad), :] * envelope)
    grid = jnp.concatenate(kernels, axis=1)
    forms = dot3((first[:, :near], first_low[:, :near]), split(grid))
    rows = []
    for chan in range(chans):
        here = slice(chan * lanes, (chan + 1) * lanes)
        real, imag = forms[:outer, here], forms[outer:, here]
        rows.append(
            jnp.concatenate(
                [real * turn[0] - imag * turn[1], real * turn[1] + imag * turn[0]], axis=1
            )
        )
    spec = dot3(split(jnp.concatenate(rows, axis=0)), (second[...], second_low[...]))
    scale = 1.0 / (outer * lanes)
    spec_real[...] = spec[:, :lanes] * scale
    spec_imag[...] = spec[:, lanes:] * scale


def convolve_kernel(
    values, spec_real, spec_imag, decay, own, first, first_low, second, second_low, back, back_low, last, last_low,
    turn, out, ordered, *, ratio
):
    outer, lanes = turn.shape[1], turn.shape[2]
    near = outer // 2
    chans = spec_real.shape[0] // outer
    peers = values.shape[0] // chans
    blocks = peers // near
    pairs = blocks // 2
    columns = []
    tile = CORES * chans
    for place, chip in enumerate(CHIP_ORDER):
        ordered[chip * tile : (chip + 1) * tile, :] = values[place * tile : (place + 1) * tile, :]
    for chan in range(chans):
        lines = ordered[pl.ds(chan, peers, stride=chans), :]
        rate = jnp.full((1, lanes), decay[own[0] + chan], F32)
        keep = jnp.exp(-rate * ratio)
        carried = [jnp.zeros((near, lanes), F32), lines[:near]]
        for block in range(1, blocks):
            carried.append(lines[block * near : (block + 1) * near] + keep * carried[-1])
        for pair in range(pairs):
            low = 2 * pair
            columns.append(
                jnp.concatenate(
                    [carried[low], carried[low + 1], carried[low + 1], carried[low + 2]], axis=0
                )
            )
    forms = dot3((first[...], first_low[...]), split(jnp.concatenate(columns, axis=1)))
    turn_real, turn_imag = turn[0], turn[1]
    rows = []
    for at in range(chans * pairs):
        here = slice(at * lanes, (at + 1) * lanes)
        real, imag = forms[:outer, here], forms[outer:, here]
        rows.append(
            jnp.concatenate(
                [real * turn_real - imag * turn_imag, real * turn_imag + imag * turn_real], axis=1
            )
        )
    spec = dot3(split(jnp.concatenate(rows, axis=0)), (second[...], second_low[...]))
    rows = []
    for at in range(chans * pairs):
        chan = at // pairs
        real = spec[at * outer : (at + 1) * outer, :lanes]
        imag = spec[at * outer : (at + 1) * outer, lanes:]
        k_real = spec_real[chan * outer : (chan + 1) * outer, :]
        k_imag = spec_imag[chan * outer : (chan + 1) * outer, :]
        rows.append(
            jnp.concatenate(
                [real * k_real - imag * k_imag, real * k_imag + imag * k_real], axis=1
            )
        )
    forms = dot3(split(jnp.concatenate(rows, axis=0)), (back[...], back_low[...]))
    columns = []
    for at in range(chans * pairs):
        real = forms[at * outer : (at + 1) * outer, :lanes]
        imag = forms[at * outer : (at + 1) * outer, lanes:]
        columns.append(
            jnp.concatenate(
                [real * turn_real + imag * turn_imag, imag * turn_real - real * turn_imag], axis=0
            )
        )
    lines = dot3((last[...], last_low[...]), split(jnp.concatenate(columns, axis=1)))
    for chan in range(chans):
        both = [
            lines[:, (chan * pairs + pair) * lanes : (chan * pairs + pair + 1) * lanes]
            for pair in range(pairs)
        ]
        ordered[pl.ds(chan, peers, stride=chans), :] = jnp.concatenate(both, axis=0)
    for place, chip in enumerate(CHIP_ORDER):
        out[place * tile : (place + 1) * tile, :] = ordered[chip * tile : (chip + 1) * tile, :]


def prepare_kernel(
    tokens, gate_w, value_w, out_w,
    value_sum, gate_sum, value_high, value_low, gate_high, gate_low, send_high, send_low, keep_high, keep_low
):
    width = tokens.shape[1]
    half = width // CORES
    me, core = lax.axis_index("chan"), core_index()
    mine = pl.ds(pl.multiple_of(me * width, width), width)
    other = pl.ds(pl.multiple_of((1 - me) * width, width), width)
    own = split(tokens[...])
    for at, part in ((0, core), (half, 1 - core)):
        here, there = slice(at, at + half), pl.ds(pl.multiple_of(part * half, half), half)
        value_sum[:, here] = dot3(own, split(value_w[mine, there]))
        gate_sum[:, here] = dot3(own, split(gate_w[mine, there]))
        value_high[:, here], value_low[:, here] = split(value_w[other, there])
        gate_high[:, here], gate_low[:, here] = split(gate_w[other, there])
        send_high[here, :], send_low[here, :] = split(out_w[there, other])
        keep_high[here, :], keep_low[here, :] = split(out_w[there, mine])


def sibling_kernel(tokens, value_in, value_high, value_low, sibling):
    half = sibling.shape[0]
    terms = split(tokens[...])
    values = value_in[:, half:] + dot3(terms, (value_high[:, half:], value_low[:, half:]))
    sibling[...] = silu(values).T


def mine_kernel(tokens, value_in, gate_in, value_high, value_low, gate_high, gate_low, merged, gated, mine, *, chans):
    half = mine.shape[0]
    terms = split(tokens[...])
    values = value_in[:, :half] + dot3(terms, (value_high[:, :half], value_low[:, :half]))
    mine[...] = silu(values).T
    gated[...] = silu(gate_in[...] + dot3(terms, (gate_high[...], gate_low[...])))
    interleave(mine, merged, core_index(), chans)


def interleave(part, merged, core, chans):
    count = part.shape[0] // chans
    for chan in range(chans):
        rows = part[pl.ds(chan, count, stride=chans), :]
        merged[pl.ds(core * chans + chan, count, stride=CORES * chans), :] = rows


def extract(merged, part, core, chans):
    count = part.shape[0] // chans
    for chan in range(chans):
        rows = merged[pl.ds(core * chans + chan, count, stride=CORES * chans), :]
        part[pl.ds(chan, count, stride=chans), :] = rows


def merge_kernel(part, _, merged, *, chans):
    interleave(part, merged, 1 - core_index(), chans)


def extract_kernel(merged, part, *, chans):
    extract(merged, part, 1 - core_index(), chans)


def first_kernel(merged, gated, send_high, send_low, keep_high, keep_low, sent, kept, mine, *, chans):
    half = mine.shape[0]
    extract(merged, mine, core_index(), chans)
    terms = split(gated[:, :half] * mine[...].T)
    sent[...] = dot3(terms, (send_high[:half, :], send_low[:half, :]))
    kept[...] = dot3(terms, (keep_high[:half, :], keep_low[:half, :]))


def send_kernel(conv, gated, part, w_high, w_low, out, term_high, term_low):
    half = conv.shape[0]
    terms = split(gated[:, half:] * conv[...].T)
    term_high[...], term_low[...] = terms
    out[...] = part[...] + dot3(terms, (w_high[half:, :], w_low[half:, :]))


def keep_kernel(term_high, term_low, part, w_high, w_low, out):
    half = term_high.shape[1]
    out[...] = part[...] + dot3((term_high[...], term_low[...]), (w_high[half:, :], w_low[half:, :]))


def angle_tables(steps, wave_numbers):
    phases = wave_numbers[:, None] * steps[None, :] % PERIOD
    angles = phases.astype(F32) * (2.0 * math.pi / PERIOD)
    return jnp.cos(angles), jnp.sin(angles)


def on_device(
    tokens,
    gate_weight,
    value_weight,
    output_weight,
    wave_numbers,
    position_in,
    bias_in,
    position_mid,
    bias_mid,
    position_out,
    decay_rate,
):
    peer_count = lax.axis_size("seq")
    row_count, local_width = tokens.shape
    seq_length = row_count * peer_count
    chans = local_width // peer_count
    near = PERIOD // row_count
    outer = 2 * near
    swap = [(0, 1), (1, 0)]
    other_tokens = lax.ppermute(tokens, "chan", swap)

    first, second, last, turn = fourier_tables(outer, row_count)
    first_h, first_l = split_table(first)
    second_h, second_l = split_table(second)
    back_h, back_l = split_table(second.T)
    last_h, last_l = split_table(last)

    me = lax.axis_index("seq")
    place_of = jnp.asarray(np.argsort(CHIP_ORDER).astype(np.int32))
    place = lax.dynamic_slice_in_dim(place_of, me // CORES, 1)
    own_first = me % CORES * (local_width // CORES) + place * chans
    cos_a, sin_a = angle_tables(jnp.arange(near, dtype=jnp.int32) * row_count, wave_numbers)
    cos_b, sin_b = angle_tables(jnp.arange(row_count, dtype=jnp.int32), wave_numbers)

    def shaped(*dims, dtype=F32):
        return jax.ShapeDtypeStruct(dims, dtype)

    width = position_in.shape[0]
    spec_real, spec_imag = call(
        lambda *refs: spectrum_kernel(*refs, seq_length=seq_length),
        [shaped(chans * outer, row_count)] * 2,
        [
            pltpu.VMEM((width, PERIOD), F32),
            pltpu.VMEM((8 * near, row_count), F32),
            pltpu.VMEM((row_count, row_count), F32),
        ],
        10**9,
        scalars={9, 10},
        name="spectrum",
    )(
        cos_a, sin_a, cos_b, sin_b, position_in, bias_in[None, :], position_mid, bias_mid[None, :], position_out,
        decay_rate, own_first, first_h, first_l, second_h, second_l, turn,
    )
    block = shaped(local_width, local_width, dtype=BF16)
    rows = shaped(row_count, local_width)
    prepared = call(prepare_kernel, [rows, rows] + [block] * 8, flops=10**9, name="prepare")(
        tokens, gate_weight, value_weight, output_weight
    )
    other_tokens, spec_real, spec_imag, prepared = lax.optimization_barrier(
        (other_tokens, spec_real, spec_imag, prepared)
    )
    (
        value_sum, gate_sum, value_high, value_low, gate_high, gate_low, send_high, send_low, keep_high, keep_low,
    ) = prepared
    weights = (value_high, value_low, gate_high, gate_low)
    flat = shaped(local_width, row_count)
    half = shaped(local_width // CORES, row_count)
    siblings = [(peer, peer ^ 1) for peer in range(peer_count)]
    same_core = [[CORES * chip + core for chip in CHIP_ORDER] for core in range(CORES)]

    def with_chans(kernel):
        return lambda *refs: kernel(*refs, chans=chans)

    sibling = call(sibling_kernel, half, flops=10**8, name="sibling")(
        other_tokens, value_sum, value_high, value_low
    )
    sibling = lax.ppermute(sibling, "seq", siblings)
    merged, gated = call(
        with_chans(mine_kernel), [flat, rows], [pltpu.VMEM(half.shape, F32)], flops=10**8, name="mine"
    )(other_tokens, value_sum, gate_sum, *weights)
    merged = call(with_chans(merge_kernel), flat, aliases={1: 0}, name="merge")(sibling, merged)
    value_lines = lax.all_to_all(
        merged, "seq", split_axis=0, concat_axis=0, tiled=True, axis_index_groups=same_core
    )
    conv_lines = call(
        lambda *refs: convolve_kernel(*refs, ratio=PERIOD / seq_length), flat, [pltpu.VMEM(flat.shape, F32)],
        flops=10**9, scalars={3, 4}, name="convolve",
    )(
        value_lines, spec_real, spec_imag, decay_rate, own_first, first_h, first_l, second_h, second_l, back_h, back_l,
        last_h, last_l, turn,
    )
    conv = lax.all_to_all(
        conv_lines, "seq", split_axis=0, concat_axis=0, tiled=True, axis_index_groups=same_core
    )
    sibling = call(with_chans(extract_kernel), half, name="extract")(conv)
    sibling = lax.ppermute(sibling, "seq", siblings)
    sent, kept = call(
        with_chans(first_kernel), [rows, rows], [pltpu.VMEM(half.shape, F32)], flops=10**8, name="first"
    )(conv, gated, send_high, send_low, keep_high, keep_low)
    term = shaped(row_count, local_width // CORES, dtype=BF16)
    sent, term_high, term_low = call(send_kernel, [rows, term, term], flops=10**8, name="send")(
        sibling, gated, sent, send_high, send_low
    )
    received = lax.ppermute(sent, "chan", swap)
    kept = call(keep_kernel, rows, flops=10**8, name="keep")(term_high, term_low, kept, keep_high, keep_low)
    return kept + received


def solution(mesh):
    placed = (
        P("seq", "chan"),
        P(None, "chan"),
        P(None, "chan"),
        P("chan", None),
        P(),
        P(),
        P(),
        P(),
        P(),
        P(None, "chan"),
        P("chan"),
    )
    return jax.shard_map(
        on_device, mesh=mesh, in_specs=placed, out_specs=P("seq", "chan"), check_vma=False
    )
```

```python
import math

import jax
import jax.numpy as jnp
import numpy as np
from jax import lax
from jax.experimental import pallas as pl
from jax.experimental.pallas import tpu as pltpu
from jax.sharding import PartitionSpec as P

PERIOD = 4096
CORES = 2
GROUP_FIRST = (43, 42)
F32 = jnp.float32
BF16 = jnp.bfloat16


def split(value):
    high = value.astype(BF16)
    low = (value - high.astype(F32)).astype(BF16)
    return high, low


def split_table(table):
    high = table.astype(np.float32).astype(jnp.bfloat16)
    low = (table - high.astype(np.float64)).astype(np.float32).astype(jnp.bfloat16)
    return high, low


def matmul(left, right):
    return jnp.dot(left, right, preferred_element_type=F32)


def dot3(left, right):
    left_high, left_low = left
    right_high, right_low = right
    return (
        matmul(left_high, right_low)
        + matmul(left_low, right_high)
        + matmul(left_high, right_high)
    )


def silu(value):
    return value / (1.0 + jnp.exp(-value))


def fourier_tables(outer, inner):
    n1 = np.arange(outer)
    n2 = np.arange(inner)
    angle = 2.0 * np.pi * ((n1[:, None] * n1[None, :]) % outer) / outer
    cos1, sin1 = np.cos(angle), np.sin(angle)
    first = np.block([[cos1, sin1], [-sin1, cos1]])
    half = outer // 2
    last = np.block([[cos1[half:], -sin1[half:]], [sin1[half:], cos1[half:]]])
    angle = 2.0 * np.pi * ((n2[:, None] * n2[None, :]) % inner) / inner
    cos2, sin2 = np.cos(angle), np.sin(angle)
    second = np.block([[cos2, -sin2], [sin2, cos2]])
    angle = 2.0 * np.pi * (n1[:, None] * n2[None, :]) / (outer * inner)
    turn = np.stack([np.cos(angle), -np.sin(angle)]).astype(np.float32)
    return first, second, last, turn


def call(kernel, out_shapes, scratch=(), flops=0, scalars=(), aliases=None, *, name):
    vmem = pl.BlockSpec(memory_space=pltpu.VMEM)
    smem = pl.BlockSpec(memory_space=pltpu.SMEM)
    many = isinstance(out_shapes, (list, tuple))

    def run(*args):
        return pl.pallas_call(
            kernel,
            out_shape=out_shapes,
            in_specs=[smem if at in scalars else vmem for at in range(len(args))],
            out_specs=[vmem] * len(out_shapes) if many else vmem,
            scratch_shapes=list(scratch),
            name=name,
            input_output_aliases=aliases or {},
            compiler_params=pltpu.CompilerParams(vmem_limit_bytes=48 << 20),
            cost_estimate=pl.CostEstimate(flops=flops, transcendentals=0, bytes_accessed=0),
        )(*args)

    return run


def core_index():
    return lax.axis_index("seq") % CORES


def group_index():
    core = core_index()
    return jnp.where(lax.axis_index("seq") // CORES == GROUP_FIRST[0], 1 - core, core)


def group_first():
    return jnp.where(group_index() == 0, GROUP_FIRST[0], GROUP_FIRST[1])


def spectrum_kernel(
    cos_a, sin_a, cos_b, sin_b, in_w, in_b, mid_w, mid_b, out_w, decay, own, first, first_low, second, second_low, turn,
    spec_real, spec_imag, features, shapes, layer, *, seq_length
):
    near, lanes = cos_a.shape[1], cos_b.shape[1]
    waves, width = cos_a.shape[0], in_w.shape[0]
    outer = turn.shape[1]
    chans = spec_real.shape[0] // outer
    own_first = own[0]
    pad = 8
    for at in range(near):
        here = slice(at * lanes, (at + 1) * lanes)
        cos_at, sin_at = cos_a[:, at : at + 1], sin_a[:, at : at + 1]
        features[:waves, here] = cos_at * cos_b[...] - sin_at * sin_b[...]
        features[waves:, here] = sin_at * cos_b[...] + cos_at * sin_b[...]
    one = (lax.broadcasted_iota(jnp.int32, (pad, PERIOD), 0) == 0).astype(F32)

    def dense(weight, bias, value):
        layer[...] = jnp.zeros_like(layer)
        layer[:width, :width] = weight[...]
        layer[width : width + 1, :width] = bias[...]
        turned = layer[...].T[:width, : width + pad]
        return jnp.maximum(dot3(split(turned), split(jnp.concatenate([value, one], axis=0))), 0.0)

    hidden = dense(in_w, in_b, features[...])
    hidden = dense(mid_w, mid_b, hidden)
    tile = out_w[:, pl.ds(pl.multiple_of(own_first // lanes * lanes, lanes), lanes)]
    own_w = pltpu.roll(tile, lanes - own_first % lanes, 1).T[:pad, :]
    lines = dot3(split(own_w), split(hidden))
    for at in range(near):
        shapes[at * pad : (at + 1) * pad, :] = lines[:, at * lanes : (at + 1) * lanes]
    spots = (
        lax.broadcasted_iota(jnp.int32, (near, lanes), 0) * lanes
        + lax.broadcasted_iota(jnp.int32, (near, lanes), 1)
    ).astype(F32) / seq_length
    kernels = []
    for chan in range(chans):
        rate = jnp.full((near, lanes), decay[own_first + chan], F32)
        envelope = jnp.exp(-rate * spots) * jnp.sqrt(2.0 * rate / seq_length)
        kernels.append(shapes[pl.ds(chan, near, stride=pad), :] * envelope)
    grid = jnp.concatenate(kernels, axis=1)
    forms = dot3((first[:, :near], first_low[:, :near]), split(grid))
    rows = []
    for chan in range(chans):
        here = slice(chan * lanes, (chan + 1) * lanes)
        real, imag = forms[:outer, here], forms[outer:, here]
        rows.append(
            jnp.concatenate(
                [real * turn[0] - imag * turn[1], real * turn[1] + imag * turn[0]], axis=1
            )
        )
    spec = dot3(split(jnp.concatenate(rows, axis=0)), (second[...], second_low[...]))
    scale = 1.0 / (outer * lanes)
    spec_real[...] = spec[:, :lanes] * scale
    spec_imag[...] = spec[:, lanes:] * scale


def convolve_kernel(
    values, spec_real, spec_imag, decay, own, first, first_low, second, second_low, back, back_low, last, last_low,
    turn, out, ordered, *, ratio
):
    outer, lanes = turn.shape[1], turn.shape[2]
    near = outer // 2
    chans = spec_real.shape[0] // outer
    peers = values.shape[0] // chans
    blocks = peers // near
    pairs = blocks // 2
    columns = []
    tile = CORES * chans
    chips = values.shape[0] // tile
    leader = group_first()

    def chip_rows(place):
        return pl.ds(pl.multiple_of((leader + place) % chips * tile, tile), tile)

    for place in range(chips):
        ordered[chip_rows(place), :] = values[place * tile : (place + 1) * tile, :]
    for chan in range(chans):
        lines = ordered[pl.ds(chan, peers, stride=chans), :]
        rate = jnp.full((1, lanes), decay[own[0] + chan], F32)
        keep = jnp.exp(-rate * ratio)
        carried = [jnp.zeros((near, lanes), F32), lines[:near]]
        for block in range(1, blocks):
            carried.append(lines[block * near : (block + 1) * near] + keep * carried[-1])
        for pair in range(pairs):
            low = 2 * pair
            columns.append(
                jnp.concatenate(
                    [carried[low], carried[low + 1], carried[low + 1], carried[low + 2]], axis=0
                )
            )
    forms = dot3((first[...], first_low[...]), split(jnp.concatenate(columns, axis=1)))
    turn_real, turn_imag = turn[0], turn[1]
    rows = []
    for at in range(chans * pairs):
        here = slice(at * lanes, (at + 1) * lanes)
        real, imag = forms[:outer, here], forms[outer:, here]
        rows.append(
            jnp.concatenate(
                [real * turn_real - imag * turn_imag, real * turn_imag + imag * turn_real], axis=1
            )
        )
    spec = dot3(split(jnp.concatenate(rows, axis=0)), (second[...], second_low[...]))
    rows = []
    for at in range(chans * pairs):
        chan = at // pairs
        real = spec[at * outer : (at + 1) * outer, :lanes]
        imag = spec[at * outer : (at + 1) * outer, lanes:]
        k_real = spec_real[chan * outer : (chan + 1) * outer, :]
        k_imag = spec_imag[chan * outer : (chan + 1) * outer, :]
        rows.append(
            jnp.concatenate(
                [real * k_real - imag * k_imag, real * k_imag + imag * k_real], axis=1
            )
        )
    forms = dot3(split(jnp.concatenate(rows, axis=0)), (back[...], back_low[...]))
    columns = []
    for at in range(chans * pairs):
        real = forms[at * outer : (at + 1) * outer, :lanes]
        imag = forms[at * outer : (at + 1) * outer, lanes:]
        columns.append(
            jnp.concatenate(
                [real * turn_real + imag * turn_imag, imag * turn_real - real * turn_imag], axis=0
            )
        )
    lines = dot3((last[...], last_low[...]), split(jnp.concatenate(columns, axis=1)))
    for chan in range(chans):
        both = [
            lines[:, (chan * pairs + pair) * lanes : (chan * pairs + pair + 1) * lanes]
            for pair in range(pairs)
        ]
        ordered[pl.ds(chan, peers, stride=chans), :] = jnp.concatenate(both, axis=0)
    for place in range(chips):
        out[place * tile : (place + 1) * tile, :] = ordered[chip_rows(place), :]


def prepare_kernel(
    tokens, gate_w, value_w, out_w,
    value_sum, gate_sum, value_high, value_low, gate_high, gate_low, send_high, send_low, keep_high, keep_low
):
    width = tokens.shape[1]
    half = width // CORES
    me, group = lax.axis_index("chan"), group_index()
    mine = pl.ds(pl.multiple_of(me * width, width), width)
    other = pl.ds(pl.multiple_of((1 - me) * width, width), width)
    own = split(tokens[...])
    for at, part in ((0, group), (half, 1 - group)):
        here, there = slice(at, at + half), pl.ds(pl.multiple_of(part * half, half), half)
        value_sum[:, here] = dot3(own, split(value_w[mine, there]))
        gate_sum[:, here] = dot3(own, split(gate_w[mine, there]))
        value_high[:, here], value_low[:, here] = split(value_w[other, there])
        gate_high[:, here], gate_low[:, here] = split(gate_w[other, there])
        send_high[here, :], send_low[here, :] = split(out_w[there, other])
        keep_high[here, :], keep_low[here, :] = split(out_w[there, mine])


def sibling_kernel(tokens, value_in, value_high, value_low, sibling):
    half = sibling.shape[0]
    terms = split(tokens[...])
    values = value_in[:, half:] + dot3(terms, (value_high[:, half:], value_low[:, half:]))
    sibling[...] = silu(values).T


def mine_kernel(tokens, value_in, gate_in, value_high, value_low, gate_high, gate_low, merged, gated, mine, *, chans):
    half = mine.shape[0]
    terms = split(tokens[...])
    values = value_in[:, :half] + dot3(terms, (value_high[:, :half], value_low[:, :half]))
    mine[...] = silu(values).T
    gated[...] = silu(gate_in[...] + dot3(terms, (gate_high[...], gate_low[...])))
    interleave(mine, merged, core_index(), chans)


def interleave(part, merged, core, chans):
    count = part.shape[0] // chans
    for chan in range(chans):
        rows = part[pl.ds(chan, count, stride=chans), :]
        merged[pl.ds(core * chans + chan, count, stride=CORES * chans), :] = rows


def extract(merged, part, core, chans):
    count = part.shape[0] // chans
    for chan in range(chans):
        rows = merged[pl.ds(core * chans + chan, count, stride=CORES * chans), :]
        part[pl.ds(chan, count, stride=chans), :] = rows


def merge_kernel(part, _, merged, *, chans):
    interleave(part, merged, 1 - core_index(), chans)


def extract_kernel(merged, part, *, chans):
    extract(merged, part, 1 - core_index(), chans)


def first_kernel(merged, gated, send_high, send_low, keep_high, keep_low, sent, kept, mine, *, chans):
    half = mine.shape[0]
    extract(merged, mine, core_index(), chans)
    terms = split(gated[:, :half] * mine[...].T)
    sent[...] = dot3(terms, (send_high[:half, :], send_low[:half, :]))
    kept[...] = dot3(terms, (keep_high[:half, :], keep_low[:half, :]))


def send_kernel(conv, gated, part, w_high, w_low, out, term_high, term_low):
    half = conv.shape[0]
    terms = split(gated[:, half:] * conv[...].T)
    term_high[...], term_low[...] = terms
    out[...] = part[...] + dot3(terms, (w_high[half:, :], w_low[half:, :]))


def keep_kernel(term_high, term_low, part, w_high, w_low, out):
    half = term_high.shape[1]
    out[...] = part[...] + dot3((term_high[...], term_low[...]), (w_high[half:, :], w_low[half:, :]))


def angle_tables(steps, wave_numbers):
    phases = wave_numbers[:, None] * steps[None, :] % PERIOD
    angles = phases.astype(F32) * (2.0 * math.pi / PERIOD)
    return jnp.cos(angles), jnp.sin(angles)


def on_device(
    tokens,
    gate_weight,
    value_weight,
    output_weight,
    wave_numbers,
    position_in,
    bias_in,
    position_mid,
    bias_mid,
    position_out,
    decay_rate,
):
    peer_count = lax.axis_size("seq")
    row_count, local_width = tokens.shape
    seq_length = row_count * peer_count
    chans = local_width // peer_count
    near = PERIOD // row_count
    outer = 2 * near
    swap = [(0, 1), (1, 0)]
    other_tokens = lax.ppermute(tokens, "chan", swap)

    first, second, last, turn = fourier_tables(outer, row_count)
    first_h, first_l = split_table(first)
    second_h, second_l = split_table(second)
    back_h, back_l = split_table(second.T)
    last_h, last_l = split_table(last)

    chip_count = peer_count // CORES
    place = (lax.axis_index("seq") // CORES - group_first() + chip_count) % chip_count
    own_first = (group_index() * (local_width // CORES) + place * chans)[None].astype(jnp.int32)
    cos_a, sin_a = angle_tables(jnp.arange(near, dtype=jnp.int32) * row_count, wave_numbers)
    cos_b, sin_b = angle_tables(jnp.arange(row_count, dtype=jnp.int32), wave_numbers)

    def shaped(*dims, dtype=F32):
        return jax.ShapeDtypeStruct(dims, dtype)

    width = position_in.shape[0]
    spec_real, spec_imag = call(
        lambda *refs: spectrum_kernel(*refs, seq_length=seq_length),
        [shaped(chans * outer, row_count)] * 2,
        [
            pltpu.VMEM((width, PERIOD), F32),
            pltpu.VMEM((8 * near, row_count), F32),
            pltpu.VMEM((row_count, row_count), F32),
        ],
        10**9,
        scalars={9, 10},
        name="spectrum",
    )(
        cos_a, sin_a, cos_b, sin_b, position_in, bias_in[None, :], position_mid, bias_mid[None, :], position_out,
        decay_rate, own_first, first_h, first_l, second_h, second_l, turn,
    )
    block = shaped(local_width, local_width, dtype=BF16)
    rows = shaped(row_count, local_width)
    prepared = call(prepare_kernel, [rows, rows] + [block] * 8, flops=10**9, name="prepare")(
        tokens, gate_weight, value_weight, output_weight
    )
    other_tokens, spec_real, spec_imag, prepared = lax.optimization_barrier(
        (other_tokens, spec_real, spec_imag, prepared)
    )
    (
        value_sum, gate_sum, value_high, value_low, gate_high, gate_low, send_high, send_low, keep_high, keep_low,
    ) = prepared
    weights = (value_high, value_low, gate_high, gate_low)
    flat = shaped(local_width, row_count)
    half = shaped(local_width // CORES, row_count)
    siblings = [(peer, peer ^ 1) for peer in range(peer_count)]
    lists = [[(first + at) % chip_count for at in range(chip_count)] for first in GROUP_FIRST]
    groups = [
        [CORES * chip + (1 - group if chip == GROUP_FIRST[0] else group) for chip in chips]
        for group, chips in enumerate(lists)
    ]

    def with_chans(kernel):
        return lambda *refs: kernel(*refs, chans=chans)

    sibling = call(sibling_kernel, half, flops=10**8, name="sibling")(
        other_tokens, value_sum, value_high, value_low
    )
    sibling = lax.ppermute(sibling, "seq", siblings)
    merged, gated = call(
        with_chans(mine_kernel), [flat, rows], [pltpu.VMEM(half.shape, F32)], flops=10**8, name="mine"
    )(other_tokens, value_sum, gate_sum, *weights)
    merged = call(with_chans(merge_kernel), flat, aliases={1: 0}, name="merge")(sibling, merged)
    value_lines = lax.all_to_all(
        merged, "seq", split_axis=0, concat_axis=0, tiled=True, axis_index_groups=groups
    )
    conv_lines = call(
        lambda *refs: convolve_kernel(*refs, ratio=PERIOD / seq_length), flat, [pltpu.VMEM(flat.shape, F32)],
        flops=10**9, scalars={3, 4}, name="convolve",
    )(
        value_lines, spec_real, spec_imag, decay_rate, own_first, first_h, first_l, second_h, second_l, back_h, back_l,
        last_h, last_l, turn,
    )
    conv = lax.all_to_all(
        conv_lines, "seq", split_axis=0, concat_axis=0, tiled=True, axis_index_groups=groups
    )
    sibling = call(with_chans(extract_kernel), half, name="extract")(conv)
    sibling = lax.ppermute(sibling, "seq", siblings)
    sent, kept = call(
        with_chans(first_kernel), [rows, rows], [pltpu.VMEM(half.shape, F32)], flops=10**8, name="first"
    )(conv, gated, send_high, send_low, keep_high, keep_low)
    term = shaped(row_count, local_width // CORES, dtype=BF16)
    sent, term_high, term_low = call(send_kernel, [rows, term, term], flops=10**8, name="send")(
        sibling, gated, sent, send_high, send_low
    )
    received = lax.ppermute(sent, "chan", swap)
    kept = call(keep_kernel, rows, flops=10**8, name="keep")(term_high, term_low, kept, keep_high, keep_low)
    return kept + received


def solution(mesh):
    placed = (
        P("seq", "chan"),
        P(None, "chan"),
        P(None, "chan"),
        P("chan", None),
        P(),
        P(),
        P(),
        P(),
        P(),
        P(None, "chan"),
        P("chan"),
    )
    return jax.shard_map(
        on_device, mesh=mesh, in_specs=placed, out_specs=P("seq", "chan"), check_vma=False
    )
```

```python
import math

import jax
import jax.numpy as jnp
import numpy as np
from jax import lax
from jax.experimental import pallas as pl
from jax.experimental.pallas import tpu as pltpu
from jax.sharding import PartitionSpec as P

PERIOD = 4096
CORES = 2
CHIP_ORDER = tuple((42 + place) % 64 for place in range(64))
F32 = jnp.float32
BF16 = jnp.bfloat16


def split(value):
    high = value.astype(BF16)
    low = (value - high.astype(F32)).astype(BF16)
    return high, low


def split_table(table):
    high = table.astype(np.float32).astype(jnp.bfloat16)
    low = (table - high.astype(np.float64)).astype(np.float32).astype(jnp.bfloat16)
    return high, low


def matmul(left, right):
    return jnp.dot(left, right, preferred_element_type=F32)


def dot3(left, right):
    left_high, left_low = left
    right_high, right_low = right
    return (
        matmul(left_high, right_low)
        + matmul(left_low, right_high)
        + matmul(left_high, right_high)
    )


def silu(value):
    return value / (1.0 + jnp.exp(-value))


def fourier_tables(outer, inner):
    n1 = np.arange(outer)
    n2 = np.arange(inner)
    angle = 2.0 * np.pi * ((n1[:, None] * n1[None, :]) % outer) / outer
    cos1, sin1 = np.cos(angle), np.sin(angle)
    first = np.block([[cos1, sin1], [-sin1, cos1]])
    half = outer // 2
    last = np.block([[cos1[half:], -sin1[half:]], [sin1[half:], cos1[half:]]])
    angle = 2.0 * np.pi * ((n2[:, None] * n2[None, :]) % inner) / inner
    cos2, sin2 = np.cos(angle), np.sin(angle)
    second = np.block([[cos2, -sin2], [sin2, cos2]])
    angle = 2.0 * np.pi * (n1[:, None] * n2[None, :]) / (outer * inner)
    turn = np.stack([np.cos(angle), -np.sin(angle)]).astype(np.float32)
    return first, second, last, turn


def call(kernel, out_shapes, scratch=(), flops=0, scalars=(), aliases=None, *, name):
    vmem = pl.BlockSpec(memory_space=pltpu.VMEM)
    smem = pl.BlockSpec(memory_space=pltpu.SMEM)
    many = isinstance(out_shapes, (list, tuple))

    def run(*args):
        return pl.pallas_call(
            kernel,
            out_shape=out_shapes,
            in_specs=[smem if at in scalars else vmem for at in range(len(args))],
            out_specs=[vmem] * len(out_shapes) if many else vmem,
            scratch_shapes=list(scratch),
            name=name,
            input_output_aliases=aliases or {},
            compiler_params=pltpu.CompilerParams(vmem_limit_bytes=48 << 20),
            cost_estimate=pl.CostEstimate(flops=flops, transcendentals=0, bytes_accessed=0),
        )(*args)

    return run


def core_index():
    return lax.axis_index("seq") % CORES


def spectrum_kernel(
    cos_a, sin_a, cos_b, sin_b, in_w, in_b, mid_w, mid_b, out_w, decay, own, first, first_low, second, second_low, turn,
    spec_real, spec_imag, features, shapes, layer, *, seq_length
):
    near, lanes = cos_a.shape[1], cos_b.shape[1]
    waves, width = cos_a.shape[0], in_w.shape[0]
    outer = turn.shape[1]
    chans = spec_real.shape[0] // outer
    own_first = own[0]
    pad = 8
    for at in range(near):
        here = slice(at * lanes, (at + 1) * lanes)
        cos_at, sin_at = cos_a[:, at : at + 1], sin_a[:, at : at + 1]
        features[:waves, here] = cos_at * cos_b[...] - sin_at * sin_b[...]
        features[waves:, here] = sin_at * cos_b[...] + cos_at * sin_b[...]
    one = (lax.broadcasted_iota(jnp.int32, (pad, PERIOD), 0) == 0).astype(F32)

    def dense(weight, bias, value):
        layer[...] = jnp.zeros_like(layer)
        layer[:width, :width] = weight[...]
        layer[width : width + 1, :width] = bias[...]
        turned = layer[...].T[:width, : width + pad]
        return jnp.maximum(dot3(split(turned), split(jnp.concatenate([value, one], axis=0))), 0.0)

    hidden = dense(in_w, in_b, features[...])
    hidden = dense(mid_w, mid_b, hidden)
    tile = out_w[:, pl.ds(pl.multiple_of(own_first // lanes * lanes, lanes), lanes)]
    own_w = pltpu.roll(tile, lanes - own_first % lanes, 1).T[:pad, :]
    lines = dot3(split(own_w), split(hidden))
    for at in range(near):
        shapes[at * pad : (at + 1) * pad, :] = lines[:, at * lanes : (at + 1) * lanes]
    spots = (
        lax.broadcasted_iota(jnp.int32, (near, lanes), 0) * lanes
        + lax.broadcasted_iota(jnp.int32, (near, lanes), 1)
    ).astype(F32) / seq_length
    kernels = []
    for chan in range(chans):
        rate = jnp.full((near, lanes), decay[own_first + chan], F32)
        envelope = jnp.exp(-rate * spots) * jnp.sqrt(2.0 * rate / seq_length)
        kernels.append(shapes[pl.ds(chan, near, stride=pad), :] * envelope)
    grid = jnp.concatenate(kernels, axis=1)
    forms = dot3((first[:, :near], first_low[:, :near]), split(grid))
    rows = []
    for chan in range(chans):
        here = slice(chan * lanes, (chan + 1) * lanes)
        real, imag = forms[:outer, here], forms[outer:, here]
        rows.append(
            jnp.concatenate(
                [real * turn[0] - imag * turn[1], real * turn[1] + imag * turn[0]], axis=1
            )
        )
    spec = dot3(split(jnp.concatenate(rows, axis=0)), (second[...], second_low[...]))
    scale = 1.0 / (outer * lanes)
    spec_real[...] = spec[:, :lanes] * scale
    spec_imag[...] = spec[:, lanes:] * scale


def convolve_kernel(
    values, spec_real, spec_imag, decay, own, first, first_low, second, second_low, back, back_low, last, last_low,
    turn, own_rows, other_rows, ordered, part, *, ratio
):
    outer, lanes = turn.shape[1], turn.shape[2]
    near = outer // 2
    chans = spec_real.shape[0] // outer
    peers = values.shape[0] // chans
    blocks = peers // near
    pairs = blocks // 2
    columns = []
    tile = CORES * chans
    for place, chip in enumerate(CHIP_ORDER):
        ordered[chip * tile : (chip + 1) * tile, :] = values[place * tile : (place + 1) * tile, :]
    for chan in range(chans):
        lines = ordered[pl.ds(chan, peers, stride=chans), :]
        rate = jnp.full((1, lanes), decay[own[0] + chan], F32)
        keep = jnp.exp(-rate * ratio)
        carried = [jnp.zeros((near, lanes), F32), lines[:near]]
        for block in range(1, blocks):
            carried.append(lines[block * near : (block + 1) * near] + keep * carried[-1])
        for pair in range(pairs):
            low = 2 * pair
            columns.append(
                jnp.concatenate(
                    [carried[low], carried[low + 1], carried[low + 1], carried[low + 2]], axis=0
                )
            )
    forms = dot3((first[...], first_low[...]), split(jnp.concatenate(columns, axis=1)))
    turn_real, turn_imag = turn[0], turn[1]
    rows = []
    for at in range(chans * pairs):
        here = slice(at * lanes, (at + 1) * lanes)
        real, imag = forms[:outer, here], forms[outer:, here]
        rows.append(
            jnp.concatenate(
                [real * turn_real - imag * turn_imag, real * turn_imag + imag * turn_real], axis=1
            )
        )
    spec = dot3(split(jnp.concatenate(rows, axis=0)), (second[...], second_low[...]))
    rows = []
    for at in range(chans * pairs):
        chan = at // pairs
        real = spec[at * outer : (at + 1) * outer, :lanes]
        imag = spec[at * outer : (at + 1) * outer, lanes:]
        k_real = spec_real[chan * outer : (chan + 1) * outer, :]
        k_imag = spec_imag[chan * outer : (chan + 1) * outer, :]
        rows.append(
            jnp.concatenate(
                [real * k_real - imag * k_imag, real * k_imag + imag * k_real], axis=1
            )
        )
    forms = dot3(split(jnp.concatenate(rows, axis=0)), (back[...], back_low[...]))
    columns = []
    for at in range(chans * pairs):
        real = forms[at * outer : (at + 1) * outer, :lanes]
        imag = forms[at * outer : (at + 1) * outer, lanes:]
        columns.append(
            jnp.concatenate(
                [real * turn_real + imag * turn_imag, imag * turn_real - real * turn_imag], axis=0
            )
        )
    lines = dot3((last[...], last_low[...]), split(jnp.concatenate(columns, axis=1)))
    for chan in range(chans):
        both = [
            lines[:, (chan * pairs + pair) * lanes : (chan * pairs + pair + 1) * lanes]
            for pair in range(pairs)
        ]
        ordered[pl.ds(chan, peers, stride=chans), :] = jnp.concatenate(both, axis=0)
    count = own_rows.shape[0]
    split_at = CHIP_ORDER[0] * chans
    core = core_index()
    for rows_of, held in ((core, own_rows), (1 - core, other_rows)):
        extract(ordered, part, rows_of, chans)
        held[: count - split_at, :] = part[split_at:, :]
        held[count - split_at :, :] = part[:split_at, :]


def prepare_kernel(
    tokens, gate_w, value_w, out_w,
    value_sum, gate_sum, value_high, value_low, gate_high, gate_low, send_high, send_low, keep_high, keep_low
):
    width = tokens.shape[1]
    half = width // CORES
    me, core = lax.axis_index("chan"), core_index()
    mine = pl.ds(pl.multiple_of(me * width, width), width)
    other = pl.ds(pl.multiple_of((1 - me) * width, width), width)
    own = split(tokens[...])
    for at, part in ((0, core), (half, 1 - core)):
        here, there = slice(at, at + half), pl.ds(pl.multiple_of(part * half, half), half)
        value_sum[:, here] = dot3(own, split(value_w[mine, there]))
        gate_sum[:, here] = dot3(own, split(gate_w[mine, there]))
        value_high[:, here], value_low[:, here] = split(value_w[other, there])
        gate_high[:, here], gate_low[:, here] = split(gate_w[other, there])
        send_high[here, :], send_low[here, :] = split(out_w[there, other])
        keep_high[here, :], keep_low[here, :] = split(out_w[there, mine])


def sibling_kernel(tokens, value_in, value_high, value_low, sibling):
    half = sibling.shape[0]
    terms = split(tokens[...])
    values = value_in[:, half:] + dot3(terms, (value_high[:, half:], value_low[:, half:]))
    sibling[...] = silu(values).T


def mine_kernel(tokens, value_in, gate_in, value_high, value_low, gate_high, gate_low, merged, gated, mine, *, chans):
    half = mine.shape[0]
    terms = split(tokens[...])
    values = value_in[:, :half] + dot3(terms, (value_high[:, :half], value_low[:, :half]))
    mine[...] = silu(values).T
    gated[...] = silu(gate_in[...] + dot3(terms, (gate_high[...], gate_low[...])))
    interleave(mine, merged, core_index(), chans)


def interleave(part, merged, core, chans):
    count = part.shape[0] // chans
    for chan in range(chans):
        rows = part[pl.ds(chan, count, stride=chans), :]
        merged[pl.ds(core * chans + chan, count, stride=CORES * chans), :] = rows


def extract(merged, part, core, chans):
    count = part.shape[0] // chans
    for chan in range(chans):
        rows = merged[pl.ds(core * chans + chan, count, stride=CORES * chans), :]
        part[pl.ds(chan, count, stride=chans), :] = rows


def merge_kernel(part, _, merged, *, chans):
    interleave(part, merged, 1 - core_index(), chans)


def join_kernel(mine, other, merged, *, chans):
    core = core_index()
    interleave(mine, merged, core, chans)
    interleave(other, merged, 1 - core, chans)


def send_kernel(conv, gated, w_high, w_low, out, term_high, term_low, part, *, chans):
    half = part.shape[0]
    core = core_index()
    for at, rows_of in ((0, core), (half, 1 - core)):
        here = slice(at, at + half)
        extract(conv, part, rows_of, chans)
        term_high[:, here], term_low[:, here] = split(gated[:, here] * part[...].T)
    out[...] = dot3((term_high[...], term_low[...]), (w_high[...], w_low[...]))


def keep_kernel(term_high, term_low, w_high, w_low, out):
    out[...] = dot3((term_high[...], term_low[...]), (w_high[...], w_low[...]))


def angle_tables(steps, wave_numbers):
    phases = wave_numbers[:, None] * steps[None, :] % PERIOD
    angles = phases.astype(F32) * (2.0 * math.pi / PERIOD)
    return jnp.cos(angles), jnp.sin(angles)


def on_device(
    tokens,
    gate_weight,
    value_weight,
    output_weight,
    wave_numbers,
    position_in,
    bias_in,
    position_mid,
    bias_mid,
    position_out,
    decay_rate,
):
    peer_count = lax.axis_size("seq")
    row_count, local_width = tokens.shape
    seq_length = row_count * peer_count
    chans = local_width // peer_count
    near = PERIOD // row_count
    outer = 2 * near
    swap = [(0, 1), (1, 0)]
    other_tokens = lax.ppermute(tokens, "chan", swap)

    first, second, last, turn = fourier_tables(outer, row_count)
    first_h, first_l = split_table(first)
    second_h, second_l = split_table(second)
    back_h, back_l = split_table(second.T)
    last_h, last_l = split_table(last)

    me = lax.axis_index("seq")
    place_of = jnp.asarray(np.argsort(CHIP_ORDER).astype(np.int32))
    place = lax.dynamic_slice_in_dim(place_of, me // CORES, 1)
    own_first = me % CORES * (local_width // CORES) + place * chans
    cos_a, sin_a = angle_tables(jnp.arange(near, dtype=jnp.int32) * row_count, wave_numbers)
    cos_b, sin_b = angle_tables(jnp.arange(row_count, dtype=jnp.int32), wave_numbers)

    def shaped(*dims, dtype=F32):
        return jax.ShapeDtypeStruct(dims, dtype)

    width = position_in.shape[0]
    spec_real, spec_imag = call(
        lambda *refs: spectrum_kernel(*refs, seq_length=seq_length),
        [shaped(chans * outer, row_count)] * 2,
        [
            pltpu.VMEM((width, PERIOD), F32),
            pltpu.VMEM((8 * near, row_count), F32),
            pltpu.VMEM((row_count, row_count), F32),
        ],
        10**9,
        scalars={9, 10},
        name="spectrum",
    )(
        cos_a, sin_a, cos_b, sin_b, position_in, bias_in[None, :], position_mid, bias_mid[None, :], position_out,
        decay_rate, own_first, first_h, first_l, second_h, second_l, turn,
    )
    block = shaped(local_width, local_width, dtype=BF16)
    rows = shaped(row_count, local_width)
    prepared = call(prepare_kernel, [rows, rows] + [block] * 8, flops=10**9, name="prepare")(
        tokens, gate_weight, value_weight, output_weight
    )
    other_tokens, spec_real, spec_imag, prepared = lax.optimization_barrier(
        (other_tokens, spec_real, spec_imag, prepared)
    )
    (
        value_sum, gate_sum, value_high, value_low, gate_high, gate_low, send_high, send_low, keep_high, keep_low,
    ) = prepared
    weights = (value_high, value_low, gate_high, gate_low)
    flat = shaped(local_width, row_count)
    half = shaped(local_width // CORES, row_count)
    siblings = [(peer, peer ^ 1) for peer in range(peer_count)]
    same_core = [[CORES * chip + core for chip in CHIP_ORDER] for core in range(CORES)]

    def with_chans(kernel):
        return lambda *refs: kernel(*refs, chans=chans)

    sibling = call(sibling_kernel, half, flops=10**8, name="sibling")(
        other_tokens, value_sum, value_high, value_low
    )
    sibling = lax.ppermute(sibling, "seq", siblings)
    merged, gated = call(
        with_chans(mine_kernel), [flat, rows], [pltpu.VMEM(half.shape, F32)], flops=10**8, name="mine"
    )(other_tokens, value_sum, gate_sum, *weights)
    merged = call(with_chans(merge_kernel), flat, aliases={1: 0}, name="merge")(sibling, merged)
    value_lines = lax.all_to_all(
        merged, "seq", split_axis=0, concat_axis=0, tiled=True, axis_index_groups=same_core
    )
    conv_own, conv_other = call(
        lambda *refs: convolve_kernel(*refs, ratio=PERIOD / seq_length), [half, half],
        [pltpu.VMEM(flat.shape, F32), pltpu.VMEM(half.shape, F32)], flops=10**9, scalars={3, 4}, name="convolve",
    )(
        value_lines, spec_real, spec_imag, decay_rate, own_first, first_h, first_l, second_h, second_l, back_h,
        back_l, last_h, last_l, turn,
    )
    conv_other = lax.ppermute(conv_other, "seq", siblings)
    conv_lines = call(with_chans(join_kernel), flat, name="join")(conv_own, conv_other)
    conv = lax.all_to_all(
        conv_lines, "seq", split_axis=0, concat_axis=0, tiled=True, axis_index_groups=same_core
    )
    term = shaped(row_count, local_width, dtype=BF16)
    sent, term_high, term_low = call(
        with_chans(send_kernel), [rows, term, term], [pltpu.VMEM(half.shape, F32)], flops=10**8, name="send"
    )(conv, gated, send_high, send_low)
    received = lax.ppermute(sent, "chan", swap)
    kept = call(keep_kernel, rows, flops=10**8, name="keep")(term_high, term_low, keep_high, keep_low)
    return kept + received


def solution(mesh):
    placed = (
        P("seq", "chan"),
        P(None, "chan"),
        P(None, "chan"),
        P("chan", None),
        P(),
        P(),
        P(),
        P(),
        P(),
        P(None, "chan"),
        P("chan"),
    )
    return jax.shard_map(
        on_device, mesh=mesh, in_specs=placed, out_specs=P("seq", "chan"), check_vma=False
    )
```

```python
import math

import jax
import jax.numpy as jnp
import numpy as np
from jax import lax
from jax.experimental import pallas as pl
from jax.experimental.pallas import tpu as pltpu
from jax.sharding import PartitionSpec as P

PERIOD = 4096
CORES = 2
CHIP_ORDER = tuple((42 + place) % 64 for place in range(64))
F32 = jnp.float32
BF16 = jnp.bfloat16


def split(value):
    high = value.astype(BF16)
    low = (value - high.astype(F32)).astype(BF16)
    return high, low


def split_table(table):
    high = table.astype(np.float32).astype(jnp.bfloat16)
    low = (table - high.astype(np.float64)).astype(np.float32).astype(jnp.bfloat16)
    return high, low


def matmul(left, right):
    return jnp.dot(left, right, preferred_element_type=F32)


def dot3(left, right):
    left_high, left_low = left
    right_high, right_low = right
    return (
        matmul(left_high, right_low)
        + matmul(left_low, right_high)
        + matmul(left_high, right_high)
    )


def packed_dot3(left, right):
    left_high, left_low = left
    right_high, right_low = right
    return matmul(
        jnp.concatenate([left_high, left_high, left_low], axis=1),
        jnp.concatenate([right_high, right_low, right_high], axis=0),
    )


def silu(value):
    return value / (1.0 + jnp.exp(-value))


def fourier_tables(outer, inner):
    n1 = np.arange(outer)
    n2 = np.arange(inner)
    angle = 2.0 * np.pi * ((n1[:, None] * n1[None, :]) % outer) / outer
    cos1, sin1 = np.cos(angle), np.sin(angle)
    first = np.block([[cos1, sin1], [-sin1, cos1]])
    half = outer // 2
    last = np.block([[cos1[half:], -sin1[half:]], [sin1[half:], cos1[half:]]])
    angle = 2.0 * np.pi * ((n2[:, None] * n2[None, :]) % inner) / inner
    cos2, sin2 = np.cos(angle), np.sin(angle)
    second = np.block([[cos2, -sin2], [sin2, cos2]])
    angle = 2.0 * np.pi * (n1[:, None] * n2[None, :]) / (outer * inner)
    turn = np.stack([np.cos(angle), -np.sin(angle)]).astype(np.float32)
    return first, second, last, turn


def call(kernel, out_shapes, scratch=(), flops=0, scalars=(), aliases=None, *, name):
    vmem = pl.BlockSpec(memory_space=pltpu.VMEM)
    smem = pl.BlockSpec(memory_space=pltpu.SMEM)
    many = isinstance(out_shapes, (list, tuple))

    def run(*args):
        return pl.pallas_call(
            kernel,
            out_shape=out_shapes,
            in_specs=[smem if at in scalars else vmem for at in range(len(args))],
            out_specs=[vmem] * len(out_shapes) if many else vmem,
            scratch_shapes=list(scratch),
            name=name,
            input_output_aliases=aliases or {},
            compiler_params=pltpu.CompilerParams(vmem_limit_bytes=48 << 20),
            cost_estimate=pl.CostEstimate(flops=flops, transcendentals=0, bytes_accessed=0),
        )(*args)

    return run


def core_index():
    return lax.axis_index("seq") % CORES


def spectrum_kernel(
    cos_a, sin_a, cos_b, sin_b, in_w, in_b, mid_w, mid_b, out_w, decay, own, first, first_low, second, second_low, turn,
    spec_real, spec_imag, features, shapes, layer, *, seq_length
):
    near, lanes = cos_a.shape[1], cos_b.shape[1]
    waves, width = cos_a.shape[0], in_w.shape[0]
    outer = turn.shape[1]
    chans = spec_real.shape[0] // outer
    own_first = own[0]
    pad = 8
    for at in range(near):
        here = slice(at * lanes, (at + 1) * lanes)
        cos_at, sin_at = cos_a[:, at : at + 1], sin_a[:, at : at + 1]
        features[:waves, here] = cos_at * cos_b[...] - sin_at * sin_b[...]
        features[waves:, here] = sin_at * cos_b[...] + cos_at * sin_b[...]
    one = (lax.broadcasted_iota(jnp.int32, (pad, PERIOD), 0) == 0).astype(F32)

    def dense(weight, bias, value):
        layer[...] = jnp.zeros_like(layer)
        layer[:width, :width] = weight[...]
        layer[width : width + 1, :width] = bias[...]
        turned = layer[...].T[:width, : width + pad]
        return jnp.maximum(dot3(split(turned), split(jnp.concatenate([value, one], axis=0))), 0.0)

    hidden = dense(in_w, in_b, features[...])
    hidden = dense(mid_w, mid_b, hidden)
    tile = out_w[:, pl.ds(pl.multiple_of(own_first // lanes * lanes, lanes), lanes)]
    own_w = pltpu.roll(tile, lanes - own_first % lanes, 1).T[:pad, :]
    lines = dot3(split(own_w), split(hidden))
    for at in range(near):
        shapes[at * pad : (at + 1) * pad, :] = lines[:, at * lanes : (at + 1) * lanes]
    spots = (
        lax.broadcasted_iota(jnp.int32, (near, lanes), 0) * lanes
        + lax.broadcasted_iota(jnp.int32, (near, lanes), 1)
    ).astype(F32) / seq_length
    kernels = []
    for chan in range(chans):
        rate = jnp.full((near, lanes), decay[own_first + chan], F32)
        envelope = jnp.exp(-rate * spots) * jnp.sqrt(2.0 * rate / seq_length)
        kernels.append(shapes[pl.ds(chan, near, stride=pad), :] * envelope)
    grid = jnp.concatenate(kernels, axis=1)
    forms = dot3((first[:, :near], first_low[:, :near]), split(grid))
    rows = []
    for chan in range(chans):
        here = slice(chan * lanes, (chan + 1) * lanes)
        real, imag = forms[:outer, here], forms[outer:, here]
        rows.append(
            jnp.concatenate(
                [real * turn[0] - imag * turn[1], real * turn[1] + imag * turn[0]], axis=1
            )
        )
    spec = dot3(split(jnp.concatenate(rows, axis=0)), (second[...], second_low[...]))
    scale = 1.0 / (outer * lanes)
    spec_real[...] = spec[:, :lanes] * scale
    spec_imag[...] = spec[:, lanes:] * scale


def convolve_kernel(
    values, spec_real, spec_imag, decay, own, first, first_low, second, second_low, back, back_low, last, last_low,
    turn, out, ordered, *, ratio
):
    outer, lanes = turn.shape[1], turn.shape[2]
    near = outer // 2
    chans = spec_real.shape[0] // outer
    peers = values.shape[0] // chans
    blocks = peers // near
    pairs = blocks // 2
    columns = []
    tile = CORES * chans
    for place, chip in enumerate(CHIP_ORDER):
        ordered[chip * tile : (chip + 1) * tile, :] = values[place * tile : (place + 1) * tile, :]
    for chan in range(chans):
        lines = ordered[pl.ds(chan, peers, stride=chans), :]
        rate = jnp.full((1, lanes), decay[own[0] + chan], F32)
        keep = jnp.exp(-rate * ratio)
        carried = [jnp.zeros((near, lanes), F32), lines[:near]]
        for block in range(1, blocks):
            carried.append(lines[block * near : (block + 1) * near] + keep * carried[-1])
        for pair in range(pairs):
            low = 2 * pair
            columns.append(
                jnp.concatenate(
                    [carried[low], carried[low + 1], carried[low + 1], carried[low + 2]], axis=0
                )
            )
    forms = packed_dot3((first[...], first_low[...]), split(jnp.concatenate(columns, axis=1)))
    turn_real, turn_imag = turn[0], turn[1]
    rows = []
    for at in range(chans * pairs):
        here = slice(at * lanes, (at + 1) * lanes)
        real, imag = forms[:outer, here], forms[outer:, here]
        rows.append(
            jnp.concatenate(
                [real * turn_real - imag * turn_imag, real * turn_imag + imag * turn_real], axis=1
            )
        )
    spec = dot3(split(jnp.concatenate(rows, axis=0)), (second[...], second_low[...]))
    rows = []
    for at in range(chans * pairs):
        chan = at // pairs
        real = spec[at * outer : (at + 1) * outer, :lanes]
        imag = spec[at * outer : (at + 1) * outer, lanes:]
        k_real = spec_real[chan * outer : (chan + 1) * outer, :]
        k_imag = spec_imag[chan * outer : (chan + 1) * outer, :]
        rows.append(
            jnp.concatenate(
                [real * k_real - imag * k_imag, real * k_imag + imag * k_real], axis=1
            )
        )
    forms = dot3(split(jnp.concatenate(rows, axis=0)), (back[...], back_low[...]))
    columns = []
    for at in range(chans * pairs):
        real = forms[at * outer : (at + 1) * outer, :lanes]
        imag = forms[at * outer : (at + 1) * outer, lanes:]
        columns.append(
            jnp.concatenate(
                [real * turn_real + imag * turn_imag, imag * turn_real - real * turn_imag], axis=0
            )
        )
    lines = packed_dot3((last[...], last_low[...]), split(jnp.concatenate(columns, axis=1)))
    for chan in range(chans):
        both = [
            lines[:, (chan * pairs + pair) * lanes : (chan * pairs + pair + 1) * lanes]
            for pair in range(pairs)
        ]
        ordered[pl.ds(chan, peers, stride=chans), :] = jnp.concatenate(both, axis=0)
    for place, chip in enumerate(CHIP_ORDER):
        out[place * tile : (place + 1) * tile, :] = ordered[chip * tile : (chip + 1) * tile, :]


def prepare_kernel(
    tokens, gate_w, value_w, out_w,
    value_sum, gate_sum, value_high, value_low, gate_high, gate_low, send_high, send_low, keep_high, keep_low
):
    width = tokens.shape[1]
    half = width // CORES
    me, core = lax.axis_index("chan"), core_index()
    mine = pl.ds(pl.multiple_of(me * width, width), width)
    other = pl.ds(pl.multiple_of((1 - me) * width, width), width)
    own = split(tokens[...])
    for at, part in ((0, core), (half, 1 - core)):
        here, there = slice(at, at + half), pl.ds(pl.multiple_of(part * half, half), half)
        value_sum[:, here] = dot3(own, split(value_w[mine, there]))
        gate_sum[:, here] = dot3(own, split(gate_w[mine, there]))
        value_high[:, here], value_low[:, here] = split(value_w[other, there])
        gate_high[:, here], gate_low[:, here] = split(gate_w[other, there])
        send_high[here, :], send_low[here, :] = split(out_w[there, other])
        keep_high[here, :], keep_low[here, :] = split(out_w[there, mine])


def sibling_kernel(tokens, value_in, value_high, value_low, sibling):
    half = sibling.shape[0]
    terms = split(tokens[...])
    values = value_in[:, half:] + dot3(terms, (value_high[:, half:], value_low[:, half:]))
    sibling[...] = silu(values).T


def mine_kernel(tokens, value_in, gate_in, value_high, value_low, gate_high, gate_low, merged, gated, mine, *, chans):
    half = mine.shape[0]
    terms = split(tokens[...])
    values = value_in[:, :half] + dot3(terms, (value_high[:, :half], value_low[:, :half]))
    mine[...] = silu(values).T
    gated[...] = silu(gate_in[...] + dot3(terms, (gate_high[...], gate_low[...])))
    interleave(mine, merged, core_index(), chans)


def interleave(part, merged, core, chans):
    count = part.shape[0] // chans
    for chan in range(chans):
        rows = part[pl.ds(chan, count, stride=chans), :]
        merged[pl.ds(core * chans + chan, count, stride=CORES * chans), :] = rows


def extract(merged, part, core, chans):
    count = part.shape[0] // chans
    for chan in range(chans):
        rows = merged[pl.ds(core * chans + chan, count, stride=CORES * chans), :]
        part[pl.ds(chan, count, stride=chans), :] = rows


def merge_kernel(part, _, merged, *, chans):
    interleave(part, merged, 1 - core_index(), chans)


def extract_kernel(merged, part, *, chans):
    extract(merged, part, 1 - core_index(), chans)


def first_kernel(merged, gated, send_high, send_low, keep_high, keep_low, sent, kept, mine, *, chans):
    half = mine.shape[0]
    extract(merged, mine, core_index(), chans)
    terms = split(gated[:, :half] * mine[...].T)
    sent[...] = dot3(terms, (send_high[:half, :], send_low[:half, :]))
    kept[...] = dot3(terms, (keep_high[:half, :], keep_low[:half, :]))


def send_kernel(conv, gated, part, w_high, w_low, out, term_high, term_low):
    half = conv.shape[0]
    terms = split(gated[:, half:] * conv[...].T)
    term_high[...], term_low[...] = terms
    out[...] = part[...] + dot3(terms, (w_high[half:, :], w_low[half:, :]))


def keep_kernel(term_high, term_low, part, w_high, w_low, out):
    half = term_high.shape[1]
    out[...] = part[...] + dot3((term_high[...], term_low[...]), (w_high[half:, :], w_low[half:, :]))


def angle_tables(steps, wave_numbers):
    phases = wave_numbers[:, None] * steps[None, :] % PERIOD
    angles = phases.astype(F32) * (2.0 * math.pi / PERIOD)
    return jnp.cos(angles), jnp.sin(angles)


def on_device(
    tokens,
    gate_weight,
    value_weight,
    output_weight,
    wave_numbers,
    position_in,
    bias_in,
    position_mid,
    bias_mid,
    position_out,
    decay_rate,
):
    peer_count = lax.axis_size("seq")
    row_count, local_width = tokens.shape
    seq_length = row_count * peer_count
    chans = local_width // peer_count
    near = PERIOD // row_count
    outer = 2 * near
    swap = [(0, 1), (1, 0)]
    other_tokens = lax.ppermute(tokens, "chan", swap)

    first, second, last, turn = fourier_tables(outer, row_count)
    first_h, first_l = split_table(first)
    second_h, second_l = split_table(second)
    back_h, back_l = split_table(second.T)
    last_h, last_l = split_table(last)

    me = lax.axis_index("seq")
    place_of = jnp.asarray(np.argsort(CHIP_ORDER).astype(np.int32))
    place = lax.dynamic_slice_in_dim(place_of, me // CORES, 1)
    own_first = me % CORES * (local_width // CORES) + place * chans
    cos_a, sin_a = angle_tables(jnp.arange(near, dtype=jnp.int32) * row_count, wave_numbers)
    cos_b, sin_b = angle_tables(jnp.arange(row_count, dtype=jnp.int32), wave_numbers)

    def shaped(*dims, dtype=F32):
        return jax.ShapeDtypeStruct(dims, dtype)

    width = position_in.shape[0]
    spec_real, spec_imag = call(
        lambda *refs: spectrum_kernel(*refs, seq_length=seq_length),
        [shaped(chans * outer, row_count)] * 2,
        [
            pltpu.VMEM((width, PERIOD), F32),
            pltpu.VMEM((8 * near, row_count), F32),
            pltpu.VMEM((row_count, row_count), F32),
        ],
        10**9,
        scalars={9, 10},
        name="spectrum",
    )(
        cos_a, sin_a, cos_b, sin_b, position_in, bias_in[None, :], position_mid, bias_mid[None, :], position_out,
        decay_rate, own_first, first_h, first_l, second_h, second_l, turn,
    )
    block = shaped(local_width, local_width, dtype=BF16)
    rows = shaped(row_count, local_width)
    prepared = call(prepare_kernel, [rows, rows] + [block] * 8, flops=10**9, name="prepare")(
        tokens, gate_weight, value_weight, output_weight
    )
    other_tokens, spec_real, spec_imag, prepared = lax.optimization_barrier(
        (other_tokens, spec_real, spec_imag, prepared)
    )
    (
        value_sum, gate_sum, value_high, value_low, gate_high, gate_low, send_high, send_low, keep_high, keep_low,
    ) = prepared
    weights = (value_high, value_low, gate_high, gate_low)
    flat = shaped(local_width, row_count)
    half = shaped(local_width // CORES, row_count)
    siblings = [(peer, peer ^ 1) for peer in range(peer_count)]
    same_core = [[CORES * chip + core for chip in CHIP_ORDER] for core in range(CORES)]

    def with_chans(kernel):
        return lambda *refs: kernel(*refs, chans=chans)

    sibling = call(sibling_kernel, half, flops=10**8, name="sibling")(
        other_tokens, value_sum, value_high, value_low
    )
    sibling = lax.ppermute(sibling, "seq", siblings)
    merged, gated = call(
        with_chans(mine_kernel), [flat, rows], [pltpu.VMEM(half.shape, F32)], flops=10**8, name="mine"
    )(other_tokens, value_sum, gate_sum, *weights)
    merged = call(with_chans(merge_kernel), flat, aliases={1: 0}, name="merge")(sibling, merged)
    value_lines = lax.all_to_all(
        merged, "seq", split_axis=0, concat_axis=0, tiled=True, axis_index_groups=same_core
    )
    conv_lines = call(
        lambda *refs: convolve_kernel(*refs, ratio=PERIOD / seq_length), flat, [pltpu.VMEM(flat.shape, F32)],
        flops=10**9, scalars={3, 4}, name="convolve",
    )(
        value_lines, spec_real, spec_imag, decay_rate, own_first, first_h, first_l, second_h, second_l, back_h, back_l,
        last_h, last_l, turn,
    )
    conv = lax.all_to_all(
        conv_lines, "seq", split_axis=0, concat_axis=0, tiled=True, axis_index_groups=same_core
    )
    sibling = call(with_chans(extract_kernel), half, name="extract")(conv)
    sibling = lax.ppermute(sibling, "seq", siblings)
    sent, kept = call(
        with_chans(first_kernel), [rows, rows], [pltpu.VMEM(half.shape, F32)], flops=10**8, name="first"
    )(conv, gated, send_high, send_low, keep_high, keep_low)
    term = shaped(row_count, local_width // CORES, dtype=BF16)
    sent, term_high, term_low = call(send_kernel, [rows, term, term], flops=10**8, name="send")(
        sibling, gated, sent, send_high, send_low
    )
    received = lax.ppermute(sent, "chan", swap)
    kept = call(keep_kernel, rows, flops=10**8, name="keep")(term_high, term_low, kept, keep_high, keep_low)
    return kept + received


def solution(mesh):
    placed = (
        P("seq", "chan"),
        P(None, "chan"),
        P(None, "chan"),
        P("chan", None),
        P(),
        P(),
        P(),
        P(),
        P(),
        P(None, "chan"),
        P("chan"),
    )
    return jax.shard_map(
        on_device, mesh=mesh, in_specs=placed, out_specs=P("seq", "chan"), check_vma=False
    )
```

```python
import math

import jax
import jax.numpy as jnp
import numpy as np
from jax import lax
from jax.experimental import pallas as pl
from jax.experimental.pallas import tpu as pltpu
from jax.sharding import PartitionSpec as P

PERIOD = 4096
CORES = 2
CHIP_ORDER = tuple((42 + place) % 64 for place in range(64))
F32 = jnp.float32
BF16 = jnp.bfloat16


def split(value):
    high = value.astype(BF16)
    low = (value - high.astype(F32)).astype(BF16)
    return high, low


def split_table(table):
    high = table.astype(np.float32).astype(jnp.bfloat16)
    low = (table - high.astype(np.float64)).astype(np.float32).astype(jnp.bfloat16)
    return high, low


def matmul(left, right):
    return jnp.dot(left, right, preferred_element_type=F32)


def dot3(left, right):
    left_high, left_low = left
    right_high, right_low = right
    return (
        matmul(left_high, right_low)
        + matmul(left_low, right_high)
        + matmul(left_high, right_high)
    )


def packed_dot3(left, right):
    left_high, left_low = left
    right_high, right_low = right
    return matmul(
        jnp.concatenate([left_high, left_high, left_low], axis=1),
        jnp.concatenate([right_high, right_low, right_high], axis=0),
    )


def silu(value):
    return value / (1.0 + jnp.exp(-value))


def fourier_tables(outer, inner):
    n1 = np.arange(outer)
    n2 = np.arange(inner)
    angle = 2.0 * np.pi * ((n1[:, None] * n1[None, :]) % outer) / outer
    cos1, sin1 = np.cos(angle), np.sin(angle)
    first = np.block([[cos1, sin1], [-sin1, cos1]])
    half = outer // 2
    last = np.block([[cos1[half:], -sin1[half:]], [sin1[half:], cos1[half:]]])
    angle = 2.0 * np.pi * ((n2[:, None] * n2[None, :]) % inner) / inner
    cos2, sin2 = np.cos(angle), np.sin(angle)
    second = np.block([[cos2, -sin2], [sin2, cos2]])
    angle = 2.0 * np.pi * (n1[:, None] * n2[None, :]) / (outer * inner)
    turn = np.stack([np.cos(angle), -np.sin(angle)]).astype(np.float32)
    return first, second, last, turn


def call(kernel, out_shapes, scratch=(), flops=0, scalars=(), aliases=None, *, name):
    vmem = pl.BlockSpec(memory_space=pltpu.VMEM)
    smem = pl.BlockSpec(memory_space=pltpu.SMEM)
    many = isinstance(out_shapes, (list, tuple))

    def run(*args):
        return pl.pallas_call(
            kernel,
            out_shape=out_shapes,
            in_specs=[smem if at in scalars else vmem for at in range(len(args))],
            out_specs=[vmem] * len(out_shapes) if many else vmem,
            scratch_shapes=list(scratch),
            name=name,
            input_output_aliases=aliases or {},
            compiler_params=pltpu.CompilerParams(vmem_limit_bytes=48 << 20),
            cost_estimate=pl.CostEstimate(flops=flops, transcendentals=0, bytes_accessed=0),
        )(*args)

    return run


def core_index():
    return lax.axis_index("seq") % CORES


def spectrum_kernel(
    cos_a, sin_a, cos_b, sin_b, in_w, in_b, mid_w, mid_b, out_w, decay, own, first, first_low, second, second_low, turn,
    spec_real, spec_imag, features, shapes, layer, *, seq_length
):
    near, lanes = cos_a.shape[1], cos_b.shape[1]
    waves, width = cos_a.shape[0], in_w.shape[0]
    outer = turn.shape[1]
    chans = spec_real.shape[0] // outer
    own_first = own[0]
    pad = 8
    for at in range(near):
        here = slice(at * lanes, (at + 1) * lanes)
        cos_at, sin_at = cos_a[:, at : at + 1], sin_a[:, at : at + 1]
        features[:waves, here] = cos_at * cos_b[...] - sin_at * sin_b[...]
        features[waves:, here] = sin_at * cos_b[...] + cos_at * sin_b[...]
    one = (lax.broadcasted_iota(jnp.int32, (pad, PERIOD), 0) == 0).astype(F32)

    def dense(weight, bias, value):
        layer[...] = jnp.zeros_like(layer)
        layer[:width, :width] = weight[...]
        layer[width : width + 1, :width] = bias[...]
        turned = layer[...].T[:width, : width + pad]
        return jnp.maximum(dot3(split(turned), split(jnp.concatenate([value, one], axis=0))), 0.0)

    hidden = dense(in_w, in_b, features[...])
    hidden = dense(mid_w, mid_b, hidden)
    tile = out_w[:, pl.ds(pl.multiple_of(own_first // lanes * lanes, lanes), lanes)]
    own_w = pltpu.roll(tile, lanes - own_first % lanes, 1).T[:pad, :]
    lines = dot3(split(own_w), split(hidden))
    for at in range(near):
        shapes[at * pad : (at + 1) * pad, :] = lines[:, at * lanes : (at + 1) * lanes]
    spots = (
        lax.broadcasted_iota(jnp.int32, (near, lanes), 0) * lanes
        + lax.broadcasted_iota(jnp.int32, (near, lanes), 1)
    ).astype(F32) / seq_length
    kernels = []
    for chan in range(chans):
        rate = jnp.full((near, lanes), decay[own_first + chan], F32)
        envelope = jnp.exp(-rate * spots) * jnp.sqrt(2.0 * rate / seq_length)
        kernels.append(shapes[pl.ds(chan, near, stride=pad), :] * envelope)
    grid = jnp.concatenate(kernels, axis=1)
    forms = dot3((first[:, :near], first_low[:, :near]), split(grid))
    rows = []
    for chan in range(chans):
        here = slice(chan * lanes, (chan + 1) * lanes)
        real, imag = forms[:outer, here], forms[outer:, here]
        rows.append(
            jnp.concatenate(
                [real * turn[0] - imag * turn[1], real * turn[1] + imag * turn[0]], axis=1
            )
        )
    spec = dot3(split(jnp.concatenate(rows, axis=0)), (second[...], second_low[...]))
    scale = 1.0 / (outer * lanes)
    spec_real[...] = spec[:, :lanes] * scale
    spec_imag[...] = spec[:, lanes:] * scale


def convolve_kernel(
    values, spec_real, spec_imag, decay, own, first, first_low, second, second_low, back, back_low, last, last_low,
    turn, out, ordered, *, ratio
):
    outer, lanes = turn.shape[1], turn.shape[2]
    near = outer // 2
    chans = spec_real.shape[0] // outer
    peers = values.shape[0] // chans
    blocks = peers // near
    pairs = blocks // 2
    columns = []
    tile = CORES * chans
    for place, chip in enumerate(CHIP_ORDER):
        ordered[chip * tile : (chip + 1) * tile, :] = values[place * tile : (place + 1) * tile, :]
    for chan in range(chans):
        lines = ordered[pl.ds(chan, peers, stride=chans), :]
        rate = jnp.full((1, lanes), decay[own[0] + chan], F32)
        keep = jnp.exp(-rate * ratio)
        carried = [jnp.zeros((near, lanes), F32), lines[:near]]
        for block in range(1, blocks):
            carried.append(lines[block * near : (block + 1) * near] + keep * carried[-1])
        for pair in range(pairs):
            low = 2 * pair
            columns.append(
                jnp.concatenate(
                    [carried[low], carried[low + 1], carried[low + 1], carried[low + 2]], axis=0
                )
            )
    forms = packed_dot3((first[...], first_low[...]), split(jnp.concatenate(columns, axis=1)))
    turn_real, turn_imag = turn[0], turn[1]
    rows = []
    for at in range(chans * pairs):
        here = slice(at * lanes, (at + 1) * lanes)
        real, imag = forms[:outer, here], forms[outer:, here]
        rows.append(
            jnp.concatenate(
                [real * turn_real - imag * turn_imag, real * turn_imag + imag * turn_real], axis=1
            )
        )
    spec = dot3(split(jnp.concatenate(rows, axis=0)), (second[...], second_low[...]))
    rows = []
    for at in range(chans * pairs):
        chan = at // pairs
        real = spec[at * outer : (at + 1) * outer, :lanes]
        imag = spec[at * outer : (at + 1) * outer, lanes:]
        k_real = spec_real[chan * outer : (chan + 1) * outer, :]
        k_imag = spec_imag[chan * outer : (chan + 1) * outer, :]
        rows.append(
            jnp.concatenate(
                [real * k_real - imag * k_imag, real * k_imag + imag * k_real], axis=1
            )
        )
    forms = dot3(split(jnp.concatenate(rows, axis=0)), (back[...], back_low[...]))
    columns = []
    for at in range(chans * pairs):
        real = forms[at * outer : (at + 1) * outer, :lanes]
        imag = forms[at * outer : (at + 1) * outer, lanes:]
        columns.append(
            jnp.concatenate(
                [real * turn_real + imag * turn_imag, imag * turn_real - real * turn_imag], axis=0
            )
        )
    lines = packed_dot3((last[...], last_low[...]), split(jnp.concatenate(columns, axis=1)))
    for chan in range(chans):
        both = [
            lines[:, (chan * pairs + pair) * lanes : (chan * pairs + pair + 1) * lanes]
            for pair in range(pairs)
        ]
        ordered[pl.ds(chan, peers, stride=chans), :] = jnp.concatenate(both, axis=0)
    for place, chip in enumerate(CHIP_ORDER):
        out[place * tile : (place + 1) * tile, :] = ordered[chip * tile : (chip + 1) * tile, :]


def prepare_kernel(
    tokens, gate_w, value_w, out_w,
    value_sum, gate_sum, value_high, value_low, gate_high, gate_low, send_high, send_low, keep_high, keep_low
):
    width = tokens.shape[1]
    half = width // CORES
    me, core = lax.axis_index("chan"), core_index()
    mine = pl.ds(pl.multiple_of(me * width, width), width)
    other = pl.ds(pl.multiple_of((1 - me) * width, width), width)
    own = split(tokens[...])
    for at, part in ((0, core), (half, 1 - core)):
        here, there = slice(at, at + half), pl.ds(pl.multiple_of(part * half, half), half)
        value_sum[:, here] = dot3(own, split(value_w[mine, there]))
        gate_sum[:, here] = dot3(own, split(gate_w[mine, there]))
        value_high[:, here], value_low[:, here] = split(value_w[other, there])
        gate_high[:, here], gate_low[:, here] = split(gate_w[other, there])
        send_high[here, :], send_low[here, :] = split(out_w[there, other])
        keep_high[here, :], keep_low[here, :] = split(out_w[there, mine])


def sibling_kernel(tokens, value_in, value_high, value_low, sibling):
    half = sibling.shape[0]
    terms = split(tokens[...])
    values = value_in[:, half:] + dot3(terms, (value_high[:, half:], value_low[:, half:]))
    sibling[...] = silu(values).T


def mine_kernel(tokens, value_in, gate_in, value_high, value_low, gate_high, gate_low, merged, gated, mine, *, chans):
    half = mine.shape[0]
    terms = split(tokens[...])
    values = value_in[:, :half] + dot3(terms, (value_high[:, :half], value_low[:, :half]))
    mine[...] = silu(values).T
    gated[...] = silu(gate_in[...] + dot3(terms, (gate_high[...], gate_low[...])))
    interleave(mine, merged, core_index(), chans)


def interleave(part, merged, core, chans):
    count = part.shape[0] // chans
    for chan in range(chans):
        rows = part[pl.ds(chan, count, stride=chans), :]
        merged[pl.ds(core * chans + chan, count, stride=CORES * chans), :] = rows


def extract(merged, part, core, chans):
    count = part.shape[0] // chans
    for chan in range(chans):
        rows = merged[pl.ds(core * chans + chan, count, stride=CORES * chans), :]
        part[pl.ds(chan, count, stride=chans), :] = rows


def merge_kernel(part, _, merged, *, chans):
    interleave(part, merged, 1 - core_index(), chans)


def extract_kernel(merged, part, *, chans):
    extract(merged, part, 1 - core_index(), chans)


def first_kernel(merged, gated, send_high, send_low, keep_high, keep_low, sent, kept, mine, *, chans):
    half = mine.shape[0]
    extract(merged, mine, core_index(), chans)
    terms = split(gated[:, :half] * mine[...].T)
    sent[...] = dot3(terms, (send_high[:half, :], send_low[:half, :]))
    kept[...] = dot3(terms, (keep_high[:half, :], keep_low[:half, :]))


def send_kernel(conv, gated, part, w_high, w_low, out, term_high, term_low):
    half = conv.shape[0]
    terms = split(gated[:, half:] * conv[...].T)
    term_high[...], term_low[...] = terms
    out[...] = part[...] + dot3(terms, (w_high[half:, :], w_low[half:, :]))


def keep_kernel(term_high, term_low, part, w_high, w_low, out):
    half = term_high.shape[1]
    out[...] = part[...] + dot3((term_high[...], term_low[...]), (w_high[half:, :], w_low[half:, :]))


def add_kernel(kept, received, out, held, sems):
    count = sems.shape[0]
    rows = held.shape[0] // count
    copies = []
    for at in range(count):
        here = pl.ds(at * rows, rows)
        held[here, :] = kept[here, :] + received[here, :]
        copies.append(pltpu.make_async_copy(held.at[here], out.at[here], sems.at[at]))
        copies[-1].start()
    for copy in copies:
        copy.wait()


def angle_tables(steps, wave_numbers):
    phases = wave_numbers[:, None] * steps[None, :] % PERIOD
    angles = phases.astype(F32) * (2.0 * math.pi / PERIOD)
    return jnp.cos(angles), jnp.sin(angles)


def on_device(
    tokens,
    gate_weight,
    value_weight,
    output_weight,
    wave_numbers,
    position_in,
    bias_in,
    position_mid,
    bias_mid,
    position_out,
    decay_rate,
):
    peer_count = lax.axis_size("seq")
    row_count, local_width = tokens.shape
    seq_length = row_count * peer_count
    chans = local_width // peer_count
    near = PERIOD // row_count
    outer = 2 * near
    swap = [(0, 1), (1, 0)]
    other_tokens = lax.ppermute(tokens, "chan", swap)

    first, second, last, turn = fourier_tables(outer, row_count)
    first_h, first_l = split_table(first)
    second_h, second_l = split_table(second)
    back_h, back_l = split_table(second.T)
    last_h, last_l = split_table(last)

    me = lax.axis_index("seq")
    place_of = jnp.asarray(np.argsort(CHIP_ORDER).astype(np.int32))
    place = lax.dynamic_slice_in_dim(place_of, me // CORES, 1)
    own_first = me % CORES * (local_width // CORES) + place * chans
    cos_a, sin_a = angle_tables(jnp.arange(near, dtype=jnp.int32) * row_count, wave_numbers)
    cos_b, sin_b = angle_tables(jnp.arange(row_count, dtype=jnp.int32), wave_numbers)

    def shaped(*dims, dtype=F32):
        return jax.ShapeDtypeStruct(dims, dtype)

    width = position_in.shape[0]
    spec_real, spec_imag = call(
        lambda *refs: spectrum_kernel(*refs, seq_length=seq_length),
        [shaped(chans * outer, row_count)] * 2,
        [
            pltpu.VMEM((width, PERIOD), F32),
            pltpu.VMEM((8 * near, row_count), F32),
            pltpu.VMEM((row_count, row_count), F32),
        ],
        10**9,
        scalars={9, 10},
        name="spectrum",
    )(
        cos_a, sin_a, cos_b, sin_b, position_in, bias_in[None, :], position_mid, bias_mid[None, :], position_out,
        decay_rate, own_first, first_h, first_l, second_h, second_l, turn,
    )
    block = shaped(local_width, local_width, dtype=BF16)
    rows = shaped(row_count, local_width)
    prepared = call(prepare_kernel, [rows, rows] + [block] * 8, flops=10**9, name="prepare")(
        tokens, gate_weight, value_weight, output_weight
    )
    other_tokens, spec_real, spec_imag, prepared = lax.optimization_barrier(
        (other_tokens, spec_real, spec_imag, prepared)
    )
    (
        value_sum, gate_sum, value_high, value_low, gate_high, gate_low, send_high, send_low, keep_high, keep_low,
    ) = prepared
    weights = (value_high, value_low, gate_high, gate_low)
    flat = shaped(local_width, row_count)
    half = shaped(local_width // CORES, row_count)
    siblings = [(peer, peer ^ 1) for peer in range(peer_count)]
    same_core = [[CORES * chip + core for chip in CHIP_ORDER] for core in range(CORES)]

    def with_chans(kernel):
        return lambda *refs: kernel(*refs, chans=chans)

    sibling = call(sibling_kernel, half, flops=10**8, name="sibling")(
        other_tokens, value_sum, value_high, value_low
    )
    sibling = lax.ppermute(sibling, "seq", siblings)
    merged, gated = call(
        with_chans(mine_kernel), [flat, rows], [pltpu.VMEM(half.shape, F32)], flops=10**8, name="mine"
    )(other_tokens, value_sum, gate_sum, *weights)
    merged = call(with_chans(merge_kernel), flat, aliases={1: 0}, name="merge")(sibling, merged)
    value_lines = lax.all_to_all(
        merged, "seq", split_axis=0, concat_axis=0, tiled=True, axis_index_groups=same_core
    )
    conv_lines = call(
        lambda *refs: convolve_kernel(*refs, ratio=PERIOD / seq_length), flat, [pltpu.VMEM(flat.shape, F32)],
        flops=10**9, scalars={3, 4}, name="convolve",
    )(
        value_lines, spec_real, spec_imag, decay_rate, own_first, first_h, first_l, second_h, second_l, back_h, back_l,
        last_h, last_l, turn,
    )
    conv = lax.all_to_all(
        conv_lines, "seq", split_axis=0, concat_axis=0, tiled=True, axis_index_groups=same_core
    )
    sibling = call(with_chans(extract_kernel), half, name="extract")(conv)
    sibling = lax.ppermute(sibling, "seq", siblings)
    sent, kept = call(
        with_chans(first_kernel), [rows, rows], [pltpu.VMEM(half.shape, F32)], flops=10**8, name="first"
    )(conv, gated, send_high, send_low, keep_high, keep_low)
    term = shaped(row_count, local_width // CORES, dtype=BF16)
    sent, term_high, term_low = call(send_kernel, [rows, term, term], flops=10**8, name="send")(
        sibling, gated, sent, send_high, send_low
    )
    received = lax.ppermute(sent, "chan", swap)
    kept = call(keep_kernel, rows, flops=10**8, name="keep")(term_high, term_low, kept, keep_high, keep_low)
    return pl.pallas_call(
        add_kernel,
        out_shape=rows,
        in_specs=[pl.BlockSpec(memory_space=pltpu.VMEM)] * 2,
        out_specs=pl.BlockSpec(memory_space=pl.ANY),
        scratch_shapes=[pltpu.VMEM(rows.shape, F32), pltpu.SemaphoreType.DMA((4,))],
        name="total",
    )(kept, received)


def solution(mesh):
    placed = (
        P("seq", "chan"),
        P(None, "chan"),
        P(None, "chan"),
        P("chan", None),
        P(),
        P(),
        P(),
        P(),
        P(),
        P(None, "chan"),
        P("chan"),
    )
    return jax.shard_map(
        on_device, mesh=mesh, in_specs=placed, out_specs=P("seq", "chan"), check_vma=False
    )
```
